128 devices in a mesh: dp: 128 (over x, z, y, core).
Axes of the slice: x: 4, y: 4, z: 4, core: 2. Of those that a mesh axis runs over, the one named last changes fastest.
Arguments:
- hidden: bfloat16 [98304, 2560], P('dp'), may hold values from -16 to 16
- rotation: bfloat16 [2560, 2560], P('dp'), may hold values from -1 to 1, as said below
- norm_gain: float32 [2, 2560], replicated, may hold values from 0.1 to 1.9
- value_weight: bfloat16 [2, 2560, 1024], P(None, None, 'dp'), may hold values from -0.125 to 0.125
- output_weight: bfloat16 [2, 1024, 2560], P(None, 'dp'), may hold values from -0.1875 to 0.1875
- lengths: int32 [128], replicated, may hold values from 1 to 768, as said below
Outputs:
- rotated_out: bfloat16 [98304, 2560], P('dp')
- calib_loss: float32 [], replicated
The draws below stay inside these ranges and needn't reach their ends.
Inputs may be any that keep to these rules, and one draw needn't show every extreme that they name: `lengths`: some device has all of its 768 rows live. `rotation`: an orthogonal matrix rounded to bfloat16.
All inputs are finite; a program needn't handle non-finite values.
Results may differ from the reference program's by a relative error of at most 0.0088.
Values may be sent and summed in bfloat16 or wider, within the bound.
A program may use at most 192 MiB of HBM per device.

```python
import jax
import jax.numpy as jnp
from jax import lax

D = 2560
E = 1024
BLOCK = 256
SLOTS = 3
LAYERS = 2
ROWS_DEV = 768
ROWS = 98304
N_DP = 128


def draw_hidden(key, part):
    noise_key, factor_key = jax.random.split(key)
    samples = jax.random.normal(noise_key, (ROWS, D), jnp.float32)
    row_factor = jnp.exp(jax.random.uniform(factor_key, (ROWS, 1), jnp.float32, -0.35, 0.35))
    rising = 0.5 + jnp.arange(ROWS, dtype=jnp.float32)[:, None] / ROWS
    return jnp.clip(samples * rising * row_factor, -16.0, 16.0).astype(jnp.bfloat16)


def draw_rotation(key, part):
    samples = jax.random.normal(key, (D, D), jnp.float32)
    orthogonal, triangle = jnp.linalg.qr(samples)
    return orthogonal.astype(jnp.bfloat16)


def draw_lengths(key, part):
    full_span = SLOTS * BLOCK
    draw_key, pick_key = jax.random.split(key)
    uniform_ints = jax.random.randint(draw_key, (N_DP,), 0, full_span)
    skewed = 1 + uniform_ints * uniform_ints // full_span
    chosen = jax.random.randint(pick_key, (), 0, N_DP)
    return jnp.where(jnp.arange(N_DP) == chosen, full_span, skewed).astype(jnp.int32)


def block_levels(key, dims, cuts, smallest, top_value):
    factor_of = 1.0
    for dim, blocks in cuts:
        draws = jax.random.uniform(jax.random.fold_in(jax.random.fold_in(key, 6), dim), (blocks,), jnp.float32, smallest / len(cuts), top_value / len(cuts))
        factor_of = factor_of * jnp.repeat(jnp.exp(draws), dims[dim] // blocks).reshape((-1,) + (1,) * (len(dims) - 1 - dim))
    return factor_of


def bell_draw(own_key, extent, deviation, bound, cuts=(), kind=jnp.bfloat16):
    loudness = block_levels(own_key, extent, cuts, -0.22, 0.18) if cuts else 1.0
    drawn = jax.random.normal(own_key, extent, jnp.float32) * deviation * loudness
    return jnp.minimum(jnp.maximum(drawn, -bound), bound).astype(kind)


def setup_inputs(seed: int = 0) -> dict:
    key_list = jax.random.split(jax.random.key(seed), 7)
    return {
        "hidden": draw_hidden(jax.random.fold_in(key_list[6], 71), 0),
        "rotation": draw_rotation(jax.random.fold_in(key_list[6], 71), 0),
        "norm_gain": jnp.clip(1.0 + 0.18 * jax.random.normal(key_list[2], (LAYERS, D), jnp.float32), 0.1, 1.9),
        "value_weight": bell_draw(key_list[3], (LAYERS, D, E), D ** -0.5, 0.125, ((2, 128),)),
        "output_weight": bell_draw(key_list[4], (LAYERS, E, D), E ** -0.5, 0.1875, ((1, 128),)),
        "lengths": draw_lengths(jax.random.fold_in(key_list[6], 71), 0),
    }


EPS_NORM = 1e-06
EPS_SCALE = 1e-06
CLIP_RATIO = 0.9
TWO_PI = 6.283185307179586

def soft_round(values):
    return values - jnp.sin(TWO_PI * values) / TWO_PI

def fake_quant(values, step_size):
    return soft_round(jnp.clip(values / step_size, -8.0, 7.0)) * step_size

def quant_columns(matrix):
    step_size = lax.optimization_barrier(jnp.max(jnp.abs(matrix), axis=0)) / 7.0 + EPS_SCALE
    return fake_quant(matrix, step_size[None, :]).astype(jnp.bfloat16)

def reference(hidden, rotation, norm_gain, value_weight, output_weight, lengths):
    positions = lax.broadcasted_iota(jnp.int32, (N_DP, ROWS_DEV), 1)
    live_rows = positions < lengths[:, None]
    count = jnp.sum(lengths).astype(jnp.float32)
    blocks = hidden.reshape(N_DP, ROWS_DEV, D)
    resid = lax.map(lambda block_rows: jnp.dot(block_rows.astype(jnp.float32), rotation.astype(jnp.float32), preferred_element_type=jnp.float32), blocks)
    loss_sum = jnp.zeros((), jnp.float32)
    for layer_number in range(LAYERS):
        scaled = (norm_gain[layer_number][:, None] * value_weight[layer_number].astype(jnp.float32)).astype(jnp.bfloat16)
        rotated_v = lax.dot_general(rotation.astype(jnp.float32), scaled.astype(jnp.float32), (((0,), (0,)), ((), ())), preferred_element_type=jnp.float32)
        value_q = quant_columns(rotated_v)
        rotated_o = jnp.dot(output_weight[layer_number].astype(jnp.float32), rotation.astype(jnp.float32), preferred_element_type=jnp.float32)
        output_q = quant_columns(rotated_o)

        def first_pass(operands):
            residual, live_mask = operands
            mean_sq = lax.optimization_barrier(jnp.mean(residual * residual, axis=1))
            normed = residual * lax.rsqrt(mean_sq + EPS_NORM)[:, None]
            step_size = CLIP_RATIO * lax.optimization_barrier(jnp.max(jnp.abs(normed), axis=1)) / 7.0 + EPS_SCALE
            act_f = fake_quant(normed, step_size[:, None])
            act_err = lax.optimization_barrier(jnp.sum((act_f - normed) * (act_f - normed), axis=1))
            mixed = jnp.dot(act_f.astype(jnp.bfloat16).astype(jnp.float32), value_q.astype(jnp.float32), preferred_element_type=jnp.float32)
            channel_top = lax.optimization_barrier(jnp.max(jnp.where(live_mask[:, None], jnp.abs(mixed), 0.0), axis=0))
            return (mean_sq, act_err, mixed, channel_top)
        mean_sq, act_err, mixed, channel_top = lax.map(first_pass, (resid, live_rows))
        vrange = lax.optimization_barrier(jnp.max(channel_top, axis=0))
        mix_step = CLIP_RATIO * vrange / 7.0 + EPS_SCALE

        def second_pass(operands):
            residual, mixed_rows = operands
            mix_f = fake_quant(mixed_rows, mix_step[None, :])
            mix_err = lax.optimization_barrier(jnp.sum((mix_f - mixed_rows) * (mix_f - mixed_rows), axis=1))
            updated = residual + jnp.dot(mix_f.astype(jnp.bfloat16).astype(jnp.float32), output_q.astype(jnp.float32), preferred_element_type=jnp.float32)
            return (updated, mix_err)
        resid, mix_err = lax.map(second_pass, (resid, mixed))
        loss_sum = loss_sum + jnp.sum(jnp.where(live_rows, mean_sq * (act_err + mix_err), 0.0))
    rotated_out = jnp.where(live_rows[:, :, None], resid, 0.0).astype(jnp.bfloat16).reshape(ROWS, D)
    return (rotated_out, loss_sum / count)
```

```python
import functools

import jax
import jax.numpy as jnp
from jax import lax
from jax.experimental import pallas as pl
from jax.experimental.pallas import tpu as pltpu
from jax.sharding import Mesh
from jax.sharding import PartitionSpec as P

DP = ("dp_0", "dp_1", "dp_2", "dp_3")
EPS_NORM = 1e-06
EPS_SCALE = 1e-06
CLIP_RATIO = 0.9
SOFT = (6.579714691285096, -12.986868668454669, 12.191614515303863, -6.570949514891455, 1.970640660123473)
ROW_STEP = 256
SUB = 16
LANES = 512
VMEM_LIMIT = 60 * 1024 * 1024


def soft_round(values):
    whole = jnp.round(values)
    rest = values - whole
    square = rest * rest
    poly = SOFT[4] * square + SOFT[3]
    for coefficient in (SOFT[2], SOFT[1], SOFT[0]):
        poly = poly * square + coefficient
    return whole + (rest * square) * poly


def fake_quant(values, step_size):
    return soft_round(jnp.clip(values / step_size, -8.0, 7.0)) * step_size


NEAR = [(dy, dc) for dy in range(4) for dc in range(2) if (dy, dc) != (0, 0)]
FAR = [(dx, dz) for dx in range(4) for dz in range(4) if (dx, dz) != (0, 0)]


def exchange_kernel(combine, x_ref, o_ref, near, mid, far, near_send, near_recv, far_send, far_recv):
    ix, iz, iy, ic = [lax.axis_index(name) for name in DP]
    near_ids = [{"dp_2": lax.rem(iy + dy, 4), "dp_3": lax.rem(ic + dc, 2)} for dy, dc in NEAR]
    far_ids = [{"dp_0": lax.rem(ix + dx, 4), "dp_1": lax.rem(iz + dz, 4)} for dx, dz in FAR]
    barrier = pltpu.get_barrier_semaphore()
    for peer in near_ids + far_ids:
        pl.semaphore_signal(barrier, inc=1, device_id=peer, device_id_type=pl.DeviceIdType.MESH)
    pl.semaphore_wait(barrier, len(NEAR) + len(FAR))

    def share(source, slots, me, ids, send, recv):
        copies = [
            pltpu.make_async_remote_copy(
                src_ref=source, dst_ref=slots.at[me], send_sem=send.at[k], recv_sem=recv.at[k],
                device_id=peer, device_id_type=pl.DeviceIdType.MESH,
            )
            for k, peer in enumerate(ids)
        ]
        for copy in copies:
            copy.start()
        slots[me] = source[...]
        for copy in copies:
            copy.wait()
        total = slots[0]
        for k in range(1, slots.shape[0]):
            total = combine(total, slots[k])
        return total

    mid[...] = share(x_ref, near, iy * 2 + ic, near_ids, near_send, near_recv)
    o_ref[...] = share(mid, far, ix * 4 + iz, far_ids, far_send, far_recv)


def exchange(combine, x, collective_id):
    shape = x.shape
    return pl.pallas_call(
        functools.partial(exchange_kernel, combine),
        out_shape=jax.ShapeDtypeStruct(shape, jnp.float32),
        in_specs=[pl.BlockSpec(memory_space=pltpu.VMEM)],
        out_specs=pl.BlockSpec(memory_space=pltpu.VMEM),
        scratch_shapes=[
            pltpu.VMEM((8,) + shape, jnp.float32),
            pltpu.VMEM(shape, jnp.float32),
            pltpu.VMEM((16,) + shape, jnp.float32),
            pltpu.SemaphoreType.DMA((len(NEAR),)),
            pltpu.SemaphoreType.DMA((len(NEAR),)),
            pltpu.SemaphoreType.DMA((len(FAR),)),
            pltpu.SemaphoreType.DMA((len(FAR),)),
        ],
        compiler_params=pltpu.CompilerParams(collective_id=collective_id, has_side_effects=True),
    )(x)


def quantize_rows(resid_ref, act_ref, square_ref, error_ref):
    width = resid_ref.shape[1]

    def step(index, carry):
        rows = pl.ds(pl.multiple_of(index * SUB, SUB), SUB)
        squares = jnp.zeros((SUB, 128), jnp.float32)
        tops = jnp.zeros((SUB, 128), jnp.float32)
        for start in range(0, width, 128):
            part = resid_ref[rows, start : start + 128]
            squares = squares + part * part
            tops = jnp.maximum(tops, jnp.abs(part))
        mean_sq = jnp.sum(squares, axis=1, keepdims=True) / width
        scale = lax.rsqrt(mean_sq + EPS_NORM)
        step_size = CLIP_RATIO * (jnp.max(tops, axis=1, keepdims=True) * scale) / 7.0 + EPS_SCALE
        gain = jnp.broadcast_to(scale / step_size, (SUB, 128))
        wide_step = jnp.broadcast_to(step_size, (SUB, 128))
        errors = jnp.zeros((SUB, 128), jnp.float32)
        for start in range(0, width, 128):
            units = resid_ref[rows, start : start + 128] * gain
            rounded = soft_round(jnp.minimum(jnp.maximum(units, -8.0), 7.0))
            gap = rounded - units
            errors = errors + gap * gap
            act_ref[rows, start : start + 128] = (rounded * wide_step).astype(jnp.bfloat16)
        square_ref[rows, :] = mean_sq
        error_ref[rows, :] = jnp.sum(errors, axis=1, keepdims=True) * (step_size * step_size)
        return carry

    lax.fori_loop(0, resid_ref.shape[0] // SUB, step, 0)


def quantize_mixed(mixed_ref, gain_ref, step_ref, mix_ref, error_ref):
    channels = mixed_ref.shape[1]

    def step(index, carry):
        rows = pl.ds(pl.multiple_of(index * SUB, SUB), SUB)
        errors = jnp.zeros((SUB, 128), jnp.float32)
        for start in range(0, channels, 128):
            cols = slice(start, start + 128)
            units = mixed_ref[rows, cols] * gain_ref[:, cols]
            rounded = soft_round(jnp.minimum(jnp.maximum(units, -8.0), 7.0))
            gap = (rounded - units) * step_ref[:, cols]
            errors = errors + gap * gap
            mix_ref[rows, cols] = (rounded * step_ref[:, cols]).astype(jnp.bfloat16)
        error_ref[rows, :] = jnp.sum(errors, axis=1, keepdims=True)
        return carry

    lax.fori_loop(0, mixed_ref.shape[0] // SUB, step, 0)


def live_column(len_ref, rows):
    first = pl.program_id(0) * rows
    return first + lax.broadcasted_iota(jnp.int32, (rows, 1), 0) < len_ref[0]


def mix_and_top(len_ref, act, vt_ref, mixed_ref, top_ref, top_buf):
    rows, channels = mixed_ref.shape
    mixed = lax.dot_general(
        act[...], vt_ref[0], (((1,), (1,)), ((), ())), preferred_element_type=jnp.float32
    )
    mixed_ref[...] = mixed
    live = live_column(len_ref, rows)
    tops = jnp.max(jnp.where(live, jnp.abs(mixed), 0.0).reshape(rows // 8, 8, channels), axis=0)

    @pl.when(pl.program_id(0) == 0)
    def _():
        top_buf[...] = tops

    @pl.when(pl.program_id(0) > 0)
    def _():
        top_buf[...] = jnp.maximum(top_buf[...], tops)

    @pl.when(pl.program_id(0) == pl.num_programs(0) - 1)
    def _():
        top_ref[...] = jnp.max(top_buf[...], axis=0, keepdims=True)


def first_kernel(len_ref, resid_ref, vt_ref, mixed_ref, square_ref, loss_ref, top_ref, act, err, top_buf):
    quantize_rows(resid_ref, act, square_ref, err)
    loss_ref[...] = square_ref[...] * err[...]
    mix_and_top(len_ref, act, vt_ref, mixed_ref, top_ref, top_buf)


def second_kernel(
    len_ref, resid_ref, mixed_ref, gain_ref, step_ref, square_ref, loss_ref, oq_ref, vt_ref,
    resid_out, mixed_out, square_out, loss_out, top_ref, mix, act, err, top_buf,
):
    quantize_mixed(mixed_ref, gain_ref, step_ref, mix, err)
    loss = loss_ref[...] + square_ref[...] * err[...]
    resid_out[...] = resid_ref[...] + jnp.dot(mix[...], oq_ref[0], preferred_element_type=jnp.float32)
    quantize_rows(resid_out, act, square_out, err)
    loss_out[...] = loss + square_out[...] * err[...]
    mix_and_top(len_ref, act, vt_ref, mixed_out, top_ref, top_buf)


def last_kernel(
    len_ref, resid_ref, mixed_ref, gain_ref, step_ref, square_ref, loss_ref, oq_ref, out_ref, sum_ref, mix, err
):
    quantize_mixed(mixed_ref, gain_ref, step_ref, mix, err)
    live = live_column(len_ref, out_ref.shape[0])
    loss = jnp.where(live, loss_ref[...] + square_ref[...] * err[...], 0.0)
    updated = resid_ref[...] + jnp.dot(mix[...], oq_ref[0], preferred_element_type=jnp.float32)
    out_ref[...] = jnp.where(live, updated, 0.0).astype(jnp.bfloat16)
    total = jnp.broadcast_to(jnp.sum(loss, axis=0, keepdims=True), sum_ref.shape)

    @pl.when(pl.program_id(0) == 0)
    def _():
        sum_ref[...] = total

    @pl.when(pl.program_id(0) > 0)
    def _():
        sum_ref[...] = sum_ref[...] + total


def row_spec(width):
    return pl.BlockSpec((ROW_STEP, width), lambda i: (i, 0))


def whole_spec(shape):
    return pl.BlockSpec(shape, lambda i: (0,) * len(shape))


def layer_spec(layer, rows, width):
    return pl.BlockSpec((1, rows, width), lambda i: (layer, 0, 0), pipeline_mode=pl.Buffered(1))


SCALAR = pl.BlockSpec(memory_space=pltpu.SMEM)


def f32(*shape):
    return jax.ShapeDtypeStruct(shape, jnp.float32)


def params():
    return pltpu.CompilerParams(vmem_limit_bytes=VMEM_LIMIT, dimension_semantics=("arbitrary",))


def first_pass(own_len, resid, value_all, layer):
    rows, width, channels = resid.shape[0], resid.shape[1], value_all.shape[1]
    return pl.pallas_call(
        first_kernel,
        grid=(rows // ROW_STEP,),
        in_specs=[SCALAR, row_spec(width), layer_spec(layer, channels, width)],
        out_specs=[row_spec(channels), row_spec(1), row_spec(1), whole_spec((1, channels))],
        out_shape=[f32(rows, channels), f32(rows, 1), f32(rows, 1), f32(1, channels)],
        scratch_shapes=[
            pltpu.VMEM((ROW_STEP, width), jnp.bfloat16),
            pltpu.VMEM((ROW_STEP, 1), jnp.float32),
            pltpu.VMEM((8, channels), jnp.float32),
        ],
        compiler_params=params(),
    )(own_len, resid, value_all)


def second_pass(own_len, resid, mixed, gain, step_size, square, loss, output_all, value_all, layer):
    rows, width, channels = resid.shape[0], resid.shape[1], value_all.shape[1]
    return pl.pallas_call(
        second_kernel,
        grid=(rows // ROW_STEP,),
        in_specs=[
            SCALAR, row_spec(width), row_spec(channels), whole_spec((1, channels)), whole_spec((1, channels)),
            row_spec(1), row_spec(1), layer_spec(layer, channels, width), layer_spec(layer + 1, channels, width),
        ],
        out_specs=[row_spec(width), row_spec(channels), row_spec(1), row_spec(1), whole_spec((1, channels))],
        out_shape=[f32(rows, width), f32(rows, channels), f32(rows, 1), f32(rows, 1), f32(1, channels)],
        scratch_shapes=[
            pltpu.VMEM((ROW_STEP, channels), jnp.bfloat16),
            pltpu.VMEM((ROW_STEP, width), jnp.bfloat16),
            pltpu.VMEM((ROW_STEP, 1), jnp.float32),
            pltpu.VMEM((8, channels), jnp.float32),
        ],
        compiler_params=params(),
    )(own_len, resid, mixed, gain, step_size, square, loss, output_all, value_all)


def last_pass(own_len, resid, mixed, gain, step_size, square, loss, output_all, layer):
    rows, width, channels = resid.shape[0], resid.shape[1], output_all.shape[1]
    return pl.pallas_call(
        last_kernel,
        grid=(rows // ROW_STEP,),
        in_specs=[
            SCALAR, row_spec(width), row_spec(channels), whole_spec((1, channels)), whole_spec((1, channels)),
            row_spec(1), row_spec(1), layer_spec(layer, channels, width),
        ],
        out_specs=[row_spec(width), whole_spec((1, 128))],
        out_shape=[jax.ShapeDtypeStruct((rows, width), jnp.bfloat16), f32(1, 128)],
        scratch_shapes=[
            pltpu.VMEM((ROW_STEP, channels), jnp.bfloat16),
            pltpu.VMEM((ROW_STEP, 1), jnp.float32),
        ],
        compiler_params=params(),
    )(own_len, resid, mixed, gain, step_size, square, loss, output_all)


def mix_scale(top):
    step_size = CLIP_RATIO * exchange(jnp.maximum, top, 1) / 7.0 + EPS_SCALE
    return 1.0 / step_size, step_size


def per_device(hidden, rotation, norm_gain, value_weight, output_weight, lengths):
    rows = hidden.shape[0]
    layers = norm_gain.shape[0]
    rotation_full = lax.all_gather(rotation, DP, axis=0, tiled=True)
    scaled = (norm_gain[:, :, None] * value_weight.astype(jnp.float32)).astype(jnp.bfloat16)
    left = jnp.concatenate(
        [hidden] + [jnp.transpose(scaled[l]) for l in range(layers)] + [output_weight[l] for l in range(layers)], axis=0
    )
    product = jnp.dot(left, rotation_full, preferred_element_type=jnp.float32)
    resid = product[:rows]
    part = value_weight.shape[2]
    value_t = product[rows : rows + layers * part].reshape(layers, part, -1)
    output = product[rows + layers * part :].reshape(layers, part, -1)
    value_tops = jnp.max(jnp.abs(value_t), axis=2, keepdims=True)
    value_q = fake_quant(value_t, value_tops / 7.0 + EPS_SCALE).astype(jnp.bfloat16)
    value_all = lax.all_gather(value_q, DP, axis=1, tiled=True)
    output_tops = exchange(jnp.maximum, jnp.max(jnp.abs(output), axis=1), 0)
    output_q = fake_quant(output, output_tops[:, None, :] / 7.0 + EPS_SCALE).astype(jnp.bfloat16)
    output_all = lax.all_gather(output_q, DP, axis=1, tiled=True)
    own_len = lax.dynamic_slice_in_dim(lengths, lax.axis_index(DP), 1)
    mixed, square, loss, top = first_pass(own_len, resid, value_all, 0)
    for layer in range(layers - 1):
        gain, step_size = mix_scale(top)
        resid, mixed, square, loss, top = second_pass(
            own_len, resid, mixed, gain, step_size, square, loss, output_all, value_all, layer
        )
    gain, step_size = mix_scale(top)
    out, local = last_pass(own_len, resid, mixed, gain, step_size, square, loss, output_all, layers - 1)
    total = exchange(jnp.add, local, 2)
    count = jnp.sum(lengths).astype(jnp.float32)
    return out, total[0, 0] / count


def solution(mesh):
    finer = Mesh(mesh.devices.reshape(4, 4, 4, 2), DP)
    in_specs = (P(DP, None), P(DP, None), P(), P(None, None, DP), P(None, DP, None), P())
    out_specs = (P(DP, None), P())
    return jax.shard_map(per_device, mesh=finer, in_specs=in_specs, out_specs=out_specs, check_vma=False)
```

```python
import functools

import jax
import jax.numpy as jnp
from jax import lax
from jax.experimental import pallas as pl
from jax.experimental.pallas import tpu as pltpu
from jax.sharding import Mesh
from jax.sharding import PartitionSpec as P

DP = ("dp_0", "dp_1", "dp_2", "dp_3")
EPS_NORM = 1e-06
EPS_SCALE = 1e-06
CLIP_RATIO = 0.9
SOFT = (6.579714691285096, -12.986868668454669, 12.191614515303863, -6.570949514891455, 1.970640660123473)
ROW_STEP = 256
SUB = 16
LANES = 512
VMEM_LIMIT = 60 * 1024 * 1024
MESH_ID = pl.DeviceIdType.MESH


def soft_round(values):
    whole = jnp.round(values)
    rest = values - whole
    square = rest * rest
    poly = SOFT[4] * square + SOFT[3]
    for coefficient in (SOFT[2], SOFT[1], SOFT[0]):
        poly = poly * square + coefficient
    return whole + (rest * square) * poly


def fake_quant(values, step_size):
    return soft_round(jnp.clip(values / step_size, -8.0, 7.0)) * step_size


NEAR = [(dy, dc) for dy in range(4) for dc in range(2) if (dy, dc) != (0, 0)]
FAR = [(dx, dz) for dx in range(4) for dz in range(4) if (dx, dz) != (0, 0)]


def exchange_kernel(combine, x_ref, o_ref, near, mid, far, near_send, near_recv, far_send, far_recv):
    ix, iz, iy, ic = [lax.axis_index(name) for name in DP]
    near_ids = [{"dp_2": lax.rem(iy + dy, 4), "dp_3": lax.rem(ic + dc, 2)} for dy, dc in NEAR]
    far_ids = [{"dp_0": lax.rem(ix + dx, 4), "dp_1": lax.rem(iz + dz, 4)} for dx, dz in FAR]
    barrier = pltpu.get_barrier_semaphore()
    for peer in near_ids + far_ids:
        pl.semaphore_signal(barrier, inc=1, device_id=peer, device_id_type=pl.DeviceIdType.MESH)
    pl.semaphore_wait(barrier, len(NEAR) + len(FAR))

    def share(source, slots, me, ids, send, recv):
        copies = [
            pltpu.make_async_remote_copy(
                src_ref=source, dst_ref=slots.at[me], send_sem=send.at[k], recv_sem=recv.at[k],
                device_id=peer, device_id_type=pl.DeviceIdType.MESH,
            )
            for k, peer in enumerate(ids)
        ]
        for copy in copies:
            copy.start()
        slots[me] = source[...]
        for copy in copies:
            copy.wait()
        total = slots[0]
        for k in range(1, slots.shape[0]):
            total = combine(total, slots[k])
        return total

    mid[...] = share(x_ref, near, iy * 2 + ic, near_ids, near_send, near_recv)
    o_ref[...] = share(mid, far, ix * 4 + iz, far_ids, far_send, far_recv)


def exchange(combine, x, collective_id):
    shape = x.shape
    return pl.pallas_call(
        functools.partial(exchange_kernel, combine),
        out_shape=jax.ShapeDtypeStruct(shape, jnp.float32),
        in_specs=[pl.BlockSpec(memory_space=pltpu.VMEM)],
        out_specs=pl.BlockSpec(memory_space=pltpu.VMEM),
        scratch_shapes=[
            pltpu.VMEM((8,) + shape, jnp.float32),
            pltpu.VMEM(shape, jnp.float32),
            pltpu.VMEM((16,) + shape, jnp.float32),
            pltpu.SemaphoreType.DMA((len(NEAR),)),
            pltpu.SemaphoreType.DMA((len(NEAR),)),
            pltpu.SemaphoreType.DMA((len(FAR),)),
            pltpu.SemaphoreType.DMA((len(FAR),)),
        ],
        compiler_params=pltpu.CompilerParams(collective_id=collective_id, has_side_effects=True),
    )(x)


RING = 4
COLORS = ((0, 1, 2), (1, 2, 0), (2, 0, 1))
PER_COLOR = 24


def places():
    return [lax.axis_index(name) for name in DP]


def neighbours(place):
    ids = []
    for axis in range(3):
        for shift in (1, RING - 1):
            ids.append({DP[axis]: lax.rem(place[axis] + shift, RING)})
    ids.append({DP[3]: 1 - place[3]})
    return ids


def greet(place):
    barrier = pltpu.get_barrier_semaphore()
    ids = neighbours(place)
    for peer in ids:
        pl.semaphore_signal(barrier, inc=1, device_id=peer, device_id_type=MESH_ID)
    return lambda: pl.semaphore_wait(barrier, len(ids))


class Gather:
    def __init__(self, buffer, place, send, recv, first_row, rows, first_column, widths):
        self.buffer, self.place, self.send, self.recv = buffer, place, send, recv
        self.half = buffer.shape[4] // 2
        self.first_row, self.rows = first_row, rows
        self.first_column, self.widths = first_column, widths
        self.partner = {DP[3]: 1 - place[3]}
        self.pending = []
        self.counter = 0

    def view(self, color, position, axis, done, part=None):
        start = self.first_column + sum(self.widths[:color])
        cols = pl.ds(pl.multiple_of(self.place[3] * self.half + start, 128), self.widths[color])
        index = [self.place[k] for k in range(3)]
        for k in done:
            index[k] = slice(None)
        index[axis] = position
        rows = pl.ds(self.first_row, self.rows)
        if part is not None:
            if done:
                index[done[0]] = pl.ds(2 * part, 2)
            else:
                cut = (self.rows // 2 + 7) // 8 * 8
                rows = pl.ds(self.first_row, cut) if part == 0 else pl.ds(self.first_row + cut, self.rows - cut)
        return self.buffer.at[index[0], index[1], index[2], rows, cols]

    def copy(self, view, peer):
        slot = self.counter
        self.counter += 1
        copy = pltpu.make_async_remote_copy(
            src_ref=view, dst_ref=view, send_sem=self.send.at[slot], recv_sem=self.recv.at[slot],
            device_id=peer, device_id_type=MESH_ID,
        )
        copy.start()
        self.pending.append((copy, peer is self.partner))
        return copy

    def steps(self):
        state = {}

        def begin(phase):
            for color, order in enumerate(COLORS):
                axis, done = order[phase], order[:phase]
                own = self.place[axis]
                up = {DP[axis]: lax.rem(own + 1, RING)}
                down = {DP[axis]: lax.rem(own + RING - 1, RING)}
                block = self.view(color, own, axis, done)
                state[phase, color] = [self.copy(block, up), self.copy(block, down)]

        def relay(phase):
            for color, order in enumerate(COLORS):
                axis, done = order[phase], order[:phase]
                own = self.place[axis]
                above, below = lax.rem(own + 1, RING), lax.rem(own + RING - 1, RING)
                from_below, from_above = state[phase, color]
                from_below.wait_recv()
                first = self.copy(self.view(color, below, axis, done, 0), {DP[axis]: above})
                self.copy(self.view(color, below, axis, done), self.partner)
                from_above.wait_recv()
                second = self.copy(self.view(color, above, axis, done, 1), {DP[axis]: below})
                self.copy(self.view(color, above, axis, done), self.partner)
                state[phase, color] = [first, second]

        def finish(phase):
            for color, order in enumerate(COLORS):
                axis, done = order[phase], order[:phase]
                across = lax.rem(self.place[axis] + 2, RING)
                for copy in state[phase, color]:
                    copy.wait_recv()
                self.copy(self.view(color, across, axis, done), self.partner)

        result = []
        for phase in range(3):
            if phase == 0:
                result.append(lambda: begin(0))
            result.append(functools.partial(relay, phase))
            if phase < 2:
                def turn(phase=phase):
                    finish(phase)
                    begin(phase + 1)
                result.append(turn)
            else:
                result.append(functools.partial(finish, phase))
        result.append(self.drain)
        return result

    def drain(self):
        for copy, kept in self.pending:
            copy.wait_send()
            if kept:
                copy.wait_recv()


def rotate_kernel(rotation_ref, hidden_ref, weight_ref, product_ref, full, left, pair, wide, send, recv, pair_send, pair_recv, local):
    place = places()
    ready = greet(place)
    rows = rotation_ref.shape[0]
    tokens = hidden_ref.shape[0]
    loads = [
        pltpu.make_async_copy(hidden_ref, left.at[pl.ds(0, tokens)], local.at[0]),
        pltpu.make_async_copy(weight_ref, left.at[pl.ds(tokens, weight_ref.shape[0])], local.at[1]),
    ]
    for load in loads:
        load.start()
    core = place[3]
    ready()
    swap = pltpu.make_async_remote_copy(
        src_ref=rotation_ref, dst_ref=pair.at[core], send_sem=pair_send, recv_sem=pair_recv,
        device_id={DP[3]: 1 - core}, device_id_type=MESH_ID,
    )
    swap.start()
    pair[core] = rotation_ref[...]
    swap.wait()
    for k in range(2):
        wide[k * rows : (k + 1) * rows, :] = pair[k].astype(jnp.float32)
    full[place[0], place[1], place[2]] = wide[...].astype(jnp.bfloat16)
    early = Gather(full, place, send.at[0], recv.at[0], 0, 2 * rows, 0, (256, 256, 256))
    late = Gather(full, place, send.at[1], recv.at[1], 0, 2 * rows, 768, (256, 128, 128))
    one, two = early.steps(), late.steps()
    for k in range(4):
        one[k]()
        two[k]()
    one[4]()
    one[5]()
    two[4]()
    for load in loads:
        load.wait()
    depth = left.shape[1]
    width = 256

    def columns(first, count):
        def body(index, carry):
            for core_half in range(2):
                cols = pl.ds(pl.multiple_of(core_half * (depth // 2) + first + index * width, width), width)
                block = full[:, :, :, :, cols].reshape(depth, width)
                product_ref[:, cols] = jnp.dot(left[...], block, preferred_element_type=jnp.float32)
            return carry

        lax.fori_loop(0, count, body, 0)

    one[6]()
    one[7]()
    columns(0, 2)
    two[5]()
    columns(512, 1)
    two[6]()
    two[7]()
    columns(768, 2)


def rotate(rotation, hidden, weights):
    rows, depth = rotation.shape
    total = hidden.shape[0] + weights.shape[0]
    return pl.pallas_call(
        rotate_kernel,
        out_shape=jax.ShapeDtypeStruct((total, depth), jnp.float32),
        in_specs=[
            pl.BlockSpec(memory_space=pltpu.VMEM),
            pl.BlockSpec(memory_space=pl.ANY),
            pl.BlockSpec(memory_space=pl.ANY),
        ],
        out_specs=pl.BlockSpec(memory_space=pltpu.VMEM),
        scratch_shapes=[
            pltpu.VMEM((RING, RING, RING, 2 * rows, depth), jnp.bfloat16),
            pltpu.VMEM((total, depth), jnp.bfloat16),
            pltpu.VMEM((2, rows, depth), jnp.bfloat16),
            pltpu.VMEM((2 * rows, depth), jnp.float32),
            pltpu.SemaphoreType.DMA((2, 63)),
            pltpu.SemaphoreType.DMA((2, 63)),
            pltpu.SemaphoreType.DMA,
            pltpu.SemaphoreType.DMA,
            pltpu.SemaphoreType.DMA((2,)),
        ],
        compiler_params=pltpu.CompilerParams(
            collective_id=3, has_side_effects=True, vmem_limit_bytes=VMEM_LIMIT
        ),
    )(rotation, hidden, weights)


def spread_kernel(shard_ref, full, send, recv, swap_send, swap_recv, local):
    place = places()
    ready = greet(place)
    count, rows = shard_ref.shape[0], shard_ref.shape[1]
    core = place[3]
    spots = [
        full.at[place[0], place[1], place[2], pl.ds(pl.multiple_of(2 * rows * k + rows * core, rows), rows)]
        for k in range(count)
    ]
    loads = [pltpu.make_async_copy(shard_ref.at[k], spots[k], local.at[k]) for k in range(count)]
    for load in loads:
        load.start()
    ready()
    swaps = []
    for k in range(count):
        loads[k].wait()
        swap = pltpu.make_async_remote_copy(
            src_ref=spots[k], dst_ref=spots[k], send_sem=swap_send.at[k], recv_sem=swap_recv.at[k],
            device_id={DP[3]: 1 - core}, device_id_type=MESH_ID,
        )
        swap.start()
        swaps.append(swap)
    for swap in swaps:
        swap.wait()
    half = count * rows
    early = Gather(full, place, send.at[0], recv.at[0], 0, half, 0, (512, 384, 384))
    late = Gather(full, place, send.at[1], recv.at[1], half, half, 0, (384, 512, 384))
    for first, second in zip(early.steps(), late.steps()):
        first()
        second()


def spread(shard):
    count, rows, depth = shard.shape
    return pl.pallas_call(
        spread_kernel,
        out_shape=jax.ShapeDtypeStruct((RING, RING, RING, 2 * rows * count, depth), jnp.bfloat16),
        in_specs=[pl.BlockSpec(memory_space=pl.ANY)],
        out_specs=pl.BlockSpec(memory_space=pltpu.VMEM),
        scratch_shapes=[
            pltpu.SemaphoreType.DMA((2, 63)),
            pltpu.SemaphoreType.DMA((2, 63)),
            pltpu.SemaphoreType.DMA((count,)),
            pltpu.SemaphoreType.DMA((count,)),
            pltpu.SemaphoreType.DMA((count,)),
        ],
        compiler_params=pltpu.CompilerParams(
            collective_id=4, has_side_effects=True, vmem_limit_bytes=VMEM_LIMIT
        ),
    )(shard)


def quantize_rows(resid_ref, act_ref, square_ref, error_ref):
    width = resid_ref.shape[1]

    def step(index, carry):
        rows = pl.ds(pl.multiple_of(index * SUB, SUB), SUB)
        squares = jnp.zeros((SUB, 128), jnp.float32)
        tops = jnp.zeros((SUB, 128), jnp.float32)
        for start in range(0, width, 128):
            part = resid_ref[rows, start : start + 128]
            squares = squares + part * part
            tops = jnp.maximum(tops, jnp.abs(part))
        mean_sq = jnp.sum(squares, axis=1, keepdims=True) / width
        scale = lax.rsqrt(mean_sq + EPS_NORM)
        step_size = CLIP_RATIO * (jnp.max(tops, axis=1, keepdims=True) * scale) / 7.0 + EPS_SCALE
        gain = jnp.broadcast_to(scale / step_size, (SUB, 128))
        wide_step = jnp.broadcast_to(step_size, (SUB, 128))
        errors = jnp.zeros((SUB, 128), jnp.float32)
        for start in range(0, width, 128):
            units = resid_ref[rows, start : start + 128] * gain
            rounded = soft_round(jnp.minimum(jnp.maximum(units, -8.0), 7.0))
            gap = rounded - units
            errors = errors + gap * gap
            act_ref[rows, start : start + 128] = (rounded * wide_step).astype(jnp.bfloat16)
        square_ref[rows, :] = mean_sq
        error_ref[rows, :] = jnp.sum(errors, axis=1, keepdims=True) * (step_size * step_size)
        return carry

    lax.fori_loop(0, resid_ref.shape[0] // SUB, step, 0)


def quantize_mixed(mixed_ref, gain_ref, step_ref, mix_ref, error_ref):
    channels = mixed_ref.shape[1]

    def step(index, carry):
        rows = pl.ds(pl.multiple_of(index * SUB, SUB), SUB)
        errors = jnp.zeros((SUB, 128), jnp.float32)
        for start in range(0, channels, 128):
            cols = slice(start, start + 128)
            units = mixed_ref[rows, cols] * gain_ref[:, cols]
            rounded = soft_round(jnp.minimum(jnp.maximum(units, -8.0), 7.0))
            gap = (rounded - units) * step_ref[:, cols]
            errors = errors + gap * gap
            mix_ref[rows, cols] = (rounded * step_ref[:, cols]).astype(jnp.bfloat16)
        error_ref[rows, :] = jnp.sum(errors, axis=1, keepdims=True)
        return carry

    lax.fori_loop(0, mixed_ref.shape[0] // SUB, step, 0)


def live_column(len_ref, rows):
    first = pl.program_id(0) * rows
    return first + lax.broadcasted_iota(jnp.int32, (rows, 1), 0) < len_ref[0]


def mix_and_top(len_ref, act, vt_ref, mixed_ref, top_ref, top_buf):
    rows, channels = mixed_ref.shape
    mixed = lax.dot_general(
        act[...], vt_ref[...].reshape(channels, act.shape[1]), (((1,), (1,)), ((), ())), preferred_element_type=jnp.float32
    )
    mixed_ref[...] = mixed
    live = live_column(len_ref, rows)
    tops = jnp.max(jnp.where(live, jnp.abs(mixed), 0.0).reshape(rows // 8, 8, channels), axis=0)

    @pl.when(pl.program_id(0) == 0)
    def _():
        top_buf[...] = tops

    @pl.when(pl.program_id(0) > 0)
    def _():
        top_buf[...] = jnp.maximum(top_buf[...], tops)

    @pl.when(pl.program_id(0) == pl.num_programs(0) - 1)
    def _():
        top_ref[...] = jnp.max(top_buf[...], axis=0, keepdims=True)


def first_kernel(len_ref, resid_ref, vt_ref, mixed_ref, square_ref, loss_ref, top_ref, act, err, top_buf):
    quantize_rows(resid_ref, act, square_ref, err)
    loss_ref[...] = square_ref[...] * err[...]
    mix_and_top(len_ref, act, vt_ref, mixed_ref, top_ref, top_buf)


def second_kernel(
    len_ref, resid_ref, mixed_ref, gain_ref, step_ref, square_ref, loss_ref, oq_ref, vt_ref,
    resid_out, mixed_out, square_out, loss_out, top_ref, mix, act, err, top_buf,
):
    quantize_mixed(mixed_ref, gain_ref, step_ref, mix, err)
    loss = loss_ref[...] + square_ref[...] * err[...]
    resid_out[...] = resid_ref[...] + jnp.dot(mix[...], oq_ref[...].reshape(mix.shape[1], oq_ref.shape[2]), preferred_element_type=jnp.float32)
    quantize_rows(resid_out, act, square_out, err)
    loss_out[...] = loss + square_out[...] * err[...]
    mix_and_top(len_ref, act, vt_ref, mixed_out, top_ref, top_buf)


def last_kernel(
    len_ref, resid_ref, mixed_ref, gain_ref, step_ref, square_ref, loss_ref, oq_ref, out_ref, sum_ref, mix, err
):
    quantize_mixed(mixed_ref, gain_ref, step_ref, mix, err)
    live = live_column(len_ref, out_ref.shape[0])
    loss = jnp.where(live, loss_ref[...] + square_ref[...] * err[...], 0.0)
    updated = resid_ref[...] + jnp.dot(mix[...], oq_ref[...].reshape(mix.shape[1], oq_ref.shape[2]), preferred_element_type=jnp.float32)
    out_ref[...] = jnp.where(live, updated, 0.0).astype(jnp.bfloat16)
    total = jnp.broadcast_to(jnp.sum(loss, axis=0, keepdims=True), sum_ref.shape)

    @pl.when(pl.program_id(0) == 0)
    def _():
        sum_ref[...] = total

    @pl.when(pl.program_id(0) > 0)
    def _():
        sum_ref[...] = sum_ref[...] + total


def row_spec(width):
    return pl.BlockSpec((ROW_STEP, width), lambda i: (i, 0))


def whole_spec(shape):
    return pl.BlockSpec(shape, lambda i: (0,) * len(shape))


def layer_spec(which, rows, width):
    return pl.BlockSpec((rows // 16, 16, width), lambda i: (0, which, 0), pipeline_mode=pl.Buffered(1))


SCALAR = pl.BlockSpec(memory_space=pltpu.SMEM)


def f32(*shape):
    return jax.ShapeDtypeStruct(shape, jnp.float32)


def params():
    return pltpu.CompilerParams(vmem_limit_bytes=VMEM_LIMIT, dimension_semantics=("arbitrary",))


def first_pass(own_len, rows, resid, weights, layer):
    width, channels = resid.shape[1], weights.shape[0] * 16
    return pl.pallas_call(
        first_kernel,
        grid=(rows // ROW_STEP,),
        in_specs=[SCALAR, row_spec(width), layer_spec(2 * layer, channels, width)],
        out_specs=[row_spec(channels), row_spec(1), row_spec(1), whole_spec((1, channels))],
        out_shape=[f32(rows, channels), f32(rows, 1), f32(rows, 1), f32(1, channels)],
        scratch_shapes=[
            pltpu.VMEM((ROW_STEP, width), jnp.bfloat16),
            pltpu.VMEM((ROW_STEP, 1), jnp.float32),
            pltpu.VMEM((8, channels), jnp.float32),
        ],
        compiler_params=params(),
    )(own_len, resid, weights)


def second_pass(own_len, rows, resid, mixed, gain, step_size, square, loss, weights, layer):
    width, channels = resid.shape[1], mixed.shape[1]
    return pl.pallas_call(
        second_kernel,
        grid=(rows // ROW_STEP,),
        in_specs=[
            SCALAR, row_spec(width), row_spec(channels), whole_spec((1, channels)), whole_spec((1, channels)),
            row_spec(1), row_spec(1), layer_spec(2 * layer + 1, channels, width), layer_spec(2 * layer + 2, channels, width),
        ],
        out_specs=[row_spec(width), row_spec(channels), row_spec(1), row_spec(1), whole_spec((1, channels))],
        out_shape=[f32(rows, width), f32(rows, channels), f32(rows, 1), f32(rows, 1), f32(1, channels)],
        scratch_shapes=[
            pltpu.VMEM((ROW_STEP, channels), jnp.bfloat16),
            pltpu.VMEM((ROW_STEP, width), jnp.bfloat16),
            pltpu.VMEM((ROW_STEP, 1), jnp.float32),
            pltpu.VMEM((8, channels), jnp.float32),
        ],
        compiler_params=params(),
    )(own_len, resid, mixed, gain, step_size, square, loss, weights, weights)


def last_pass(own_len, rows, resid, mixed, gain, step_size, square, loss, weights, layer):
    width, channels = resid.shape[1], mixed.shape[1]
    return pl.pallas_call(
        last_kernel,
        grid=(rows // ROW_STEP,),
        in_specs=[
            SCALAR, row_spec(width), row_spec(channels), whole_spec((1, channels)), whole_spec((1, channels)),
            row_spec(1), row_spec(1), layer_spec(2 * layer + 1, channels, width),
        ],
        out_specs=[row_spec(width), whole_spec((1, 128))],
        out_shape=[jax.ShapeDtypeStruct((rows, width), jnp.bfloat16), f32(1, 128)],
        scratch_shapes=[
            pltpu.VMEM((ROW_STEP, channels), jnp.bfloat16),
            pltpu.VMEM((ROW_STEP, 1), jnp.float32),
        ],
        compiler_params=params(),
    )(own_len, resid, mixed, gain, step_size, square, loss, weights)


def mix_scale(top):
    step_size = CLIP_RATIO * exchange(jnp.maximum, top, 1) / 7.0 + EPS_SCALE
    return 1.0 / step_size, step_size


def per_device(hidden, rotation, norm_gain, value_weight, output_weight, lengths):
    rows, width = hidden.shape
    layers, part = output_weight.shape[0], output_weight.shape[1]
    scaled = (norm_gain[:, :, None] * value_weight.astype(jnp.float32)).astype(jnp.bfloat16)
    own = jnp.stack([jnp.transpose(scaled, (0, 2, 1)), output_weight], axis=1)
    product = rotate(rotation, hidden, own.reshape(2 * layers * part, width))
    turned = product[rows:].reshape(layers, 2, part, width)
    value_t, output = turned[:, 0], turned[:, 1]
    output_tops = exchange(jnp.maximum, jnp.max(jnp.abs(output), axis=1), 0)
    value_tops = jnp.max(jnp.abs(value_t), axis=2, keepdims=True)
    value_q = fake_quant(value_t, value_tops / 7.0 + EPS_SCALE)
    output_q = fake_quant(output, output_tops[:, None, :] / 7.0 + EPS_SCALE)
    shard = jnp.stack([value_q, output_q], axis=1).astype(jnp.bfloat16).reshape(2 * layers, part, width)
    weights = spread(shard).reshape(RING**3, 4 * layers * part, width)
    own_len = lax.dynamic_slice_in_dim(lengths, lax.axis_index(DP), 1)
    resid = product
    mixed, square, loss, top = first_pass(own_len, rows, resid, weights, 0)
    for layer in range(layers - 1):
        gain, step_size = mix_scale(top)
        resid, mixed, square, loss, top = second_pass(
            own_len, rows, resid, mixed, gain, step_size, square, loss, weights, layer
        )
    gain, step_size = mix_scale(top)
    out, local = last_pass(own_len, rows, resid, mixed, gain, step_size, square, loss, weights, layers - 1)
    total = exchange(jnp.add, local, 2)
    count = jnp.sum(lengths).astype(jnp.float32)
    return out, total[0, 0] / count


def solution(mesh):
    finer = Mesh(mesh.devices.reshape(4, 4, 4, 2), DP)
    in_specs = (P(DP, None), P(DP, None), P(), P(None, None, DP), P(None, DP, None), P())
    out_specs = (P(DP, None), P())
    return jax.shard_map(per_device, mesh=finer, in_specs=in_specs, out_specs=out_specs, check_vma=False)
```

```python
import functools

import jax
import jax.numpy as jnp
from jax import lax
from jax.experimental import pallas as pl
from jax.experimental.pallas import tpu as pltpu
from jax.sharding import Mesh
from jax.sharding import PartitionSpec as P

DP = ("dp_0", "dp_1", "dp_2", "dp_3")
EPS_NORM = 1e-06
EPS_SCALE = 1e-06
CLIP_RATIO = 0.9
SOFT = (6.579714691285096, -12.986868668454669, 12.191614515303863, -6.570949514891455, 1.970640660123473)
ROW_STEP = 256
SUB = 64
VMEM_LIMIT = 60 * 1024 * 1024
MESH_ID = pl.DeviceIdType.MESH


def soft_round(values):
    whole = jnp.round(values)
    rest = values - whole
    square = rest * rest
    poly = SOFT[4] * square + SOFT[3]
    for coefficient in (SOFT[2], SOFT[1], SOFT[0]):
        poly = poly * square + coefficient
    return whole + (rest * square) * poly


def fake_quant(values, step_size):
    return soft_round(jnp.clip(values / step_size, -8.0, 7.0)) * step_size


RING = 4
COLORS = ((0, 1, 2), (1, 2, 0), (2, 0, 1))
PER_COLOR = 24


def places():
    return [lax.axis_index(name) for name in DP]


def neighbours(place):
    ids = []
    for axis in range(3):
        for shift in (1, RING - 1):
            ids.append({DP[axis]: lax.rem(place[axis] + shift, RING)})
    ids.append({DP[3]: 1 - place[3]})
    return ids


def greet(place):
    barrier = pltpu.get_barrier_semaphore()
    ids = neighbours(place)
    for peer in ids:
        pl.semaphore_signal(barrier, inc=1, device_id=peer, device_id_type=MESH_ID)
    return lambda: pl.semaphore_wait(barrier, len(ids))


class Gather:
    def __init__(self, buffer, place, send, recv, first_row, rows, first_column, widths):
        self.buffer, self.place, self.send, self.recv = buffer, place, send, recv
        self.half = buffer.shape[4] // 2
        self.first_row, self.rows = first_row, rows
        self.first_column, self.widths = first_column, widths
        self.partner = {DP[3]: 1 - place[3]}
        self.pending = []
        self.counter = 0

    def view(self, color, position, axis, done, part=None):
        start = self.first_column + sum(self.widths[:color])
        cols = pl.ds(pl.multiple_of(self.place[3] * self.half + start, 128), self.widths[color])
        index = [self.place[k] for k in range(3)]
        for k in done:
            index[k] = slice(None)
        index[axis] = position
        rows = pl.ds(self.first_row, self.rows)
        if part is not None:
            if done:
                index[done[0]] = pl.ds(2 * part, 2)
            else:
                cut = (self.rows // 2 + 7) // 8 * 8
                rows = pl.ds(self.first_row, cut) if part == 0 else pl.ds(self.first_row + cut, self.rows - cut)
        return self.buffer.at[index[0], index[1], index[2], rows, cols]

    def copy(self, view, peer):
        slot = self.counter
        self.counter += 1
        copy = pltpu.make_async_remote_copy(
            src_ref=view, dst_ref=view, send_sem=self.send.at[slot], recv_sem=self.recv.at[slot],
            device_id=peer, device_id_type=MESH_ID,
        )
        copy.start()
        self.pending.append((copy, peer is self.partner))
        return copy

    def steps(self):
        state = {}

        def begin(phase):
            for color, order in enumerate(COLORS):
                axis, done = order[phase], order[:phase]
                own = self.place[axis]
                up = {DP[axis]: lax.rem(own + 1, RING)}
                down = {DP[axis]: lax.rem(own + RING - 1, RING)}
                block = self.view(color, own, axis, done)
                state[phase, color] = [self.copy(block, up), self.copy(block, down)]

        def relay(phase):
            for color, order in enumerate(COLORS):
                axis, done = order[phase], order[:phase]
                own = self.place[axis]
                above, below = lax.rem(own + 1, RING), lax.rem(own + RING - 1, RING)
                from_below, from_above = state[phase, color]
                from_below.wait_recv()
                first = self.copy(self.view(color, below, axis, done, 0), {DP[axis]: above})
                self.copy(self.view(color, below, axis, done), self.partner)
                from_above.wait_recv()
                second = self.copy(self.view(color, above, axis, done, 1), {DP[axis]: below})
                self.copy(self.view(color, above, axis, done), self.partner)
                state[phase, color] = [first, second]

        def finish(phase):
            for color, order in enumerate(COLORS):
                axis, done = order[phase], order[:phase]
                across = lax.rem(self.place[axis] + 2, RING)
                for copy in state[phase, color]:
                    copy.wait_recv()
                self.copy(self.view(color, across, axis, done), self.partner)

        result = []
        for phase in range(3):
            if phase == 0:
                result.append(lambda: begin(0))
            result.append(functools.partial(relay, phase))
            if phase < 2:
                def turn(phase=phase):
                    finish(phase)
                    begin(phase + 1)
                result.append(turn)
            else:
                result.append(functools.partial(finish, phase))
        result.append(self.drain)
        return result

    def drain(self):
        for copy, kept in self.pending:
            copy.wait_send()
            if kept:
                copy.wait_recv()


def rotate_kernel(rotation_ref, hidden_ref, weight_ref, product_ref, full, left, pair, wide, send, recv, pair_send, pair_recv, local):
    place = places()
    ready = greet(place)
    rows = rotation_ref.shape[0]
    tokens = hidden_ref.shape[0]
    loads = [
        pltpu.make_async_copy(hidden_ref, left.at[pl.ds(0, tokens)], local.at[0]),
        pltpu.make_async_copy(weight_ref, left.at[pl.ds(tokens, weight_ref.shape[0])], local.at[1]),
    ]
    for load in loads:
        load.start()
    core = place[3]
    ready()
    swap = pltpu.make_async_remote_copy(
        src_ref=rotation_ref, dst_ref=pair.at[core], send_sem=pair_send, recv_sem=pair_recv,
        device_id={DP[3]: 1 - core}, device_id_type=MESH_ID,
    )
    swap.start()
    pair[core] = rotation_ref[...]
    swap.wait()
    for k in range(2):
        wide[k * rows : (k + 1) * rows, :] = pair[k].astype(jnp.float32)
    full[place[0], place[1], place[2]] = wide[...].astype(jnp.bfloat16)
    early = Gather(full, place, send.at[0], recv.at[0], 0, 2 * rows, 0, (256, 256, 256))
    late = Gather(full, place, send.at[1], recv.at[1], 0, 2 * rows, 768, (256, 128, 128))
    one, two = early.steps(), late.steps()
    for k in range(4):
        one[k]()
        two[k]()
    one[4]()
    one[5]()
    two[4]()
    for load in loads:
        load.wait()
    depth = left.shape[1]
    width = 256

    def columns(first, count):
        def body(index, carry):
            for core_half in range(2):
                cols = pl.ds(pl.multiple_of(core_half * (depth // 2) + first + index * width, width), width)
                block = full[:, :, :, :, cols].reshape(depth, width)
                product_ref[:, cols] = jnp.dot(left[...], block, preferred_element_type=jnp.float32)
            return carry

        lax.fori_loop(0, count, body, 0)

    one[6]()
    one[7]()
    columns(0, 2)
    two[5]()
    columns(512, 1)
    two[6]()
    two[7]()
    columns(768, 2)


def rotate(rotation, hidden, weights):
    rows, depth = rotation.shape
    total = hidden.shape[0] + weights.shape[0]
    return pl.pallas_call(
        rotate_kernel,
        out_shape=jax.ShapeDtypeStruct((total, depth), jnp.float32),
        in_specs=[
            pl.BlockSpec(memory_space=pltpu.VMEM),
            pl.BlockSpec(memory_space=pl.ANY),
            pl.BlockSpec(memory_space=pl.ANY),
        ],
        out_specs=pl.BlockSpec(memory_space=pltpu.VMEM),
        scratch_shapes=[
            pltpu.VMEM((RING, RING, RING, 2 * rows, depth), jnp.bfloat16),
            pltpu.VMEM((total, depth), jnp.bfloat16),
            pltpu.VMEM((2, rows, depth), jnp.bfloat16),
            pltpu.VMEM((2 * rows, depth), jnp.float32),
            pltpu.SemaphoreType.DMA((2, 63)),
            pltpu.SemaphoreType.DMA((2, 63)),
            pltpu.SemaphoreType.DMA,
            pltpu.SemaphoreType.DMA,
            pltpu.SemaphoreType.DMA((2,)),
        ],
        compiler_params=pltpu.CompilerParams(
            collective_id=3, has_side_effects=True, vmem_limit_bytes=VMEM_LIMIT
        ),
    )(rotation, hidden, weights)


NEAR = [(dy, dc) for dy in range(4) for dc in range(2) if (dy, dc) != (0, 0)]
FAR = [(dx, dz) for dx in range(4) for dz in range(4) if (dx, dz) != (0, 0)]


def near_peers(place):
    return [{DP[2]: lax.rem(place[2] + dy, 4), DP[3]: lax.rem(place[3] + dc, 2)} for dy, dc in NEAR]


def far_peers(place):
    return [{DP[0]: lax.rem(place[0] + dx, 4), DP[1]: lax.rem(place[1] + dz, 4)} for dx, dz in FAR]


class Exchange:
    def __init__(self, combine, place, buffers):
        self.combine, self.place = combine, place
        self.source, self.near, self.mid, self.far = buffers[:4]
        self.near_send, self.near_recv, self.far_send, self.far_recv = buffers[4:]

    def share(self, source, slots, me, peers, send, recv):
        slots[me] = source[...]
        copies = [
            pltpu.make_async_remote_copy(
                src_ref=source, dst_ref=slots.at[me], send_sem=send.at[k], recv_sem=recv.at[k],
                device_id=peer, device_id_type=MESH_ID,
            )
            for k, peer in enumerate(peers)
        ]
        for copy in copies:
            copy.start()
        return copies

    def total(self, slots, copies):
        for copy in copies:
            copy.wait()
        result = slots[0]
        for k in range(1, slots.shape[0]):
            result = self.combine(result, slots[k])
        return result

    def start(self, value):
        self.source[...] = value
        me = self.place[2] * 2 + self.place[3]
        self.copies = self.share(self.source, self.near, me, near_peers(self.place), self.near_send, self.near_recv)

    def turn(self):
        self.mid[...] = self.total(self.near, self.copies)
        me = self.place[0] * 4 + self.place[1]
        self.copies = self.share(self.mid, self.far, me, far_peers(self.place), self.far_send, self.far_recv)

    def finish(self):
        return self.total(self.far, self.copies)


def exchange_scratch(shape):
    return [
        pltpu.VMEM(shape, jnp.float32),
        pltpu.VMEM((8,) + shape, jnp.float32),
        pltpu.VMEM(shape, jnp.float32),
        pltpu.VMEM((16,) + shape, jnp.float32),
        pltpu.SemaphoreType.DMA((len(NEAR),)),
        pltpu.SemaphoreType.DMA((len(NEAR),)),
        pltpu.SemaphoreType.DMA((len(FAR),)),
        pltpu.SemaphoreType.DMA((len(FAR),)),
    ]


def quantize_rows(resid, act, square, error, first, count):
    width = resid.shape[1]

    def step(index, carry):
        rows = pl.ds(pl.multiple_of(first + index * SUB, SUB), SUB)
        squares = jnp.zeros((SUB, 128), jnp.float32)
        tops = jnp.zeros((SUB, 128), jnp.float32)
        for start in range(0, width, 128):
            part = resid[rows, start : start + 128]
            squares = squares + part * part
            tops = jnp.maximum(tops, jnp.abs(part))
        mean_sq = jnp.sum(squares, axis=1, keepdims=True) / width
        scale = lax.rsqrt(mean_sq + EPS_NORM)
        step_size = CLIP_RATIO * (jnp.max(tops, axis=1, keepdims=True) * scale) / 7.0 + EPS_SCALE
        gain = jnp.broadcast_to(scale / step_size, (SUB, 128))
        wide_step = jnp.broadcast_to(step_size, (SUB, 128))
        errors = jnp.zeros((SUB, 128), jnp.float32)
        for start in range(0, width, 128):
            units = resid[rows, start : start + 128] * gain
            rounded = soft_round(jnp.minimum(jnp.maximum(units, -8.0), 7.0))
            gap = rounded - units
            errors = errors + gap * gap
            act[rows, start : start + 128] = (rounded * wide_step).astype(jnp.bfloat16)
        square[rows, :] = mean_sq
        error[rows, :] = jnp.sum(errors, axis=1, keepdims=True) * (step_size * step_size)
        return carry

    lax.fori_loop(0, count // SUB, step, 0)


def quantize_mixed(mixed, gain, step_size, mix, error, first, count):
    channels = mixed.shape[1]

    def step(index, carry):
        rows = pl.ds(pl.multiple_of(first + index * SUB, SUB), SUB)
        errors = jnp.zeros((SUB, 128), jnp.float32)
        for start in range(0, channels, 128):
            cols = slice(start, start + 128)
            units = mixed[rows, cols] * gain[:, cols]
            rounded = soft_round(jnp.minimum(jnp.maximum(units, -8.0), 7.0))
            gap = (rounded - units) * step_size[:, cols]
            errors = errors + gap * gap
            mix[rows, cols] = (rounded * step_size[:, cols]).astype(jnp.bfloat16)
        error[rows, :] = jnp.sum(errors, axis=1, keepdims=True)
        return carry

    lax.fori_loop(0, count // SUB, step, 0)


def layers_kernel(
    len_ref, product_ref, out_ref, sum_ref,
    full, resid, act, mixed, mix, pair, turned, square, error, loss, top, gain, step_size,
    ring_send, ring_recv, swap_send, swap_recv, local, *exchanges,
):
    place = places()
    core = place[3]
    tokens, width = resid.shape
    channels = mixed.shape[1]
    part = pair.shape[2]
    barrier = pltpu.get_barrier_semaphore()
    peers = near_peers(place) + far_peers(place)
    for peer in peers:
        pl.semaphore_signal(barrier, inc=1, device_id=peer, device_id_type=MESH_ID)
    loads = [
        pltpu.make_async_copy(product_ref.at[pl.ds(tokens, 4 * part)], turned, local.at[0]),
        pltpu.make_async_copy(product_ref.at[pl.ds(0, tokens)], resid, local.at[1]),
    ]
    for load in loads:
        load.start()
    tops_max = Exchange(jnp.maximum, place, exchanges[0:8])
    ranges = [Exchange(jnp.maximum, place, exchanges[8:16]), Exchange(jnp.maximum, place, exchanges[16:24])]
    loss_sum = Exchange(jnp.add, place, exchanges[24:32])

    def matrix(which):
        return turned[which * part : (which + 1) * part, :]

    def swap(first):
        copy = pltpu.make_async_remote_copy(
            src_ref=pair.at[core, pl.ds(first, 2)], dst_ref=pair.at[core, pl.ds(first, 2)],
            send_sem=swap_send.at[first // 2], recv_sem=swap_recv.at[first // 2],
            device_id={DP[3]: 1 - core}, device_id_type=MESH_ID,
        )
        copy.start()
        return copy

    def combine(first):
        for k in (first, first + 1):
            both = jnp.concatenate([pair[0, k].astype(jnp.float32), pair[1, k].astype(jnp.float32)], axis=0)
            full[place[0], place[1], place[2], 2 * part * k : 2 * part * (k + 1), :] = both.astype(jnp.bfloat16)

    def weights(which):
        return full[:, :, :, 2 * part * which : 2 * part * (which + 1), :].reshape(channels, width)

    loads[0].wait()
    for k in range(2):
        value = matrix(k)
        value_top = jnp.max(jnp.abs(value), axis=1, keepdims=True)
        pair[core, k] = fake_quant(value, value_top / 7.0 + EPS_SCALE).astype(jnp.bfloat16)
    output_tops = jnp.concatenate(
        [jnp.max(jnp.abs(matrix(k)), axis=0, keepdims=True) for k in (2, 3)], axis=0
    )
    pl.semaphore_wait(barrier, len(peers))
    swapped = swap(0)
    tops_max.start(output_tops)
    values = Gather(full, place, ring_send.at[0], ring_recv.at[0], 0, 4 * part, 0, (512, 384, 384)).steps()
    outputs = Gather(full, place, ring_send.at[1], ring_recv.at[1], 4 * part, 4 * part, 0, (384, 512, 384)).steps()
    loads[1].wait()
    swapped.wait()
    combine(0)
    done = 0

    def rows_ahead(count):
        nonlocal done
        quantize_rows(resid, act, square, error, done, count)
        done = done + count

    values[0]()
    rows_ahead(128)
    values[1]()
    tops_max.turn()
    rows_ahead(64)
    values[2]()
    rows_ahead(128)
    values[3]()
    tops = tops_max.finish()
    for k in (2, 3):
        step = tops[k - 2 : k - 1, :] / 7.0 + EPS_SCALE
        pair[core, k] = fake_quant(matrix(k), step).astype(jnp.bfloat16)
    swapped = swap(2)
    rows_ahead(64)
    swapped.wait()
    combine(2)
    values[4]()
    outputs[0]()
    rows_ahead(128)
    outputs[1]()
    rows_ahead(128)
    outputs[2]()
    rows_ahead(128)
    outputs[3]()
    values[5]()
    outputs[4]()
    values[6]()
    values[7]()

    def live_rows(first, count):
        return first + lax.broadcasted_iota(jnp.int32, (count, 1), 0) < len_ref[0]

    def mix_block(first, which):
        rows = pl.ds(pl.multiple_of(first, ROW_STEP), ROW_STEP)
        block = lax.dot_general(
            act[rows, :], weights(which), (((1,), (1,)), ((), ())), preferred_element_type=jnp.float32
        )
        mixed[rows, :] = block
        seen = jnp.where(live_rows(first, ROW_STEP), jnp.abs(block), 0.0)
        top[...] = jnp.maximum(top[...], jnp.max(seen.reshape(ROW_STEP // 8, 8, channels), axis=0))

    def set_steps(vrange):
        sizes = CLIP_RATIO * vrange / 7.0 + EPS_SCALE
        step_size[...] = sizes
        gain[...] = 1.0 / sizes

    top[...] = jnp.zeros_like(top)
    loss[...] = square[...] * error[...]
    blocks = tokens // ROW_STEP
    lax.fori_loop(0, 1, lambda i, c: (mix_block(i * ROW_STEP, 0), c)[1], 0)
    outputs[5]()
    lax.fori_loop(1, blocks, lambda i, c: (mix_block(i * ROW_STEP, 0), c)[1], 0)
    ranges[0].start(jnp.max(top[...], axis=0, keepdims=True))
    outputs[6]()
    ranges[0].turn()
    outputs[7]()
    set_steps(ranges[0].finish())
    top[...] = jnp.zeros_like(top)

    def middle(index, carry):
        first = index * ROW_STEP
        rows = pl.ds(pl.multiple_of(first, ROW_STEP), ROW_STEP)
        quantize_mixed(mixed, gain, step_size, mix, error, first, ROW_STEP)
        loss[rows, :] = loss[rows, :] + square[rows, :] * error[rows, :]
        resid[rows, :] = resid[rows, :] + jnp.dot(mix[rows, :], weights(2), preferred_element_type=jnp.float32)
        quantize_rows(resid, act, square, error, first, ROW_STEP)
        loss[rows, :] = loss[rows, :] + square[rows, :] * error[rows, :]
        mix_block(first, 1)
        return carry

    lax.fori_loop(0, blocks, middle, 0)
    ranges[1].start(jnp.max(top[...], axis=0, keepdims=True))
    ranges[1].turn()
    set_steps(ranges[1].finish())
    quantize_mixed(mixed, gain, step_size, mix, error, 0, tokens)
    kept = jnp.where(live_rows(0, tokens), loss[...] + square[...] * error[...], 0.0)
    loss_sum.start(jnp.broadcast_to(jnp.sum(kept, axis=0, keepdims=True), sum_ref.shape))

    def last(index, carry):
        first = index * ROW_STEP
        rows = pl.ds(pl.multiple_of(first, ROW_STEP), ROW_STEP)
        updated = resid[rows, :] + jnp.dot(mix[rows, :], weights(3), preferred_element_type=jnp.float32)
        out_ref[rows, :] = jnp.where(live_rows(first, ROW_STEP), updated, 0.0).astype(jnp.bfloat16)
        return carry

    lax.fori_loop(0, 1, last, 0)
    loss_sum.turn()
    lax.fori_loop(1, blocks, last, 0)
    sum_ref[...] = loss_sum.finish()


def run_layers(own_len, product, tokens, channels, part):
    width = product.shape[1]
    column = pltpu.VMEM((tokens, 1), jnp.float32)
    scratch = [
        pltpu.VMEM((RING, RING, RING, 8 * part, width), jnp.bfloat16),
        pltpu.VMEM((tokens, width), jnp.float32),
        pltpu.VMEM((tokens, width), jnp.bfloat16),
        pltpu.VMEM((tokens, channels), jnp.float32),
        pltpu.VMEM((tokens, channels), jnp.bfloat16),
        pltpu.VMEM((2, 4, part, width), jnp.bfloat16),
        pltpu.VMEM((4 * part, width), jnp.float32),
        column, column, column,
        pltpu.VMEM((8, channels), jnp.float32),
        pltpu.VMEM((1, channels), jnp.float32),
        pltpu.VMEM((1, channels), jnp.float32),
        pltpu.SemaphoreType.DMA((2, 63)),
        pltpu.SemaphoreType.DMA((2, 63)),
        pltpu.SemaphoreType.DMA((2,)),
        pltpu.SemaphoreType.DMA((2,)),
        pltpu.SemaphoreType.DMA((2,)),
    ]
    for shape in ((2, width), (1, channels), (1, channels), (1, 128)):
        scratch = scratch + exchange_scratch(shape)
    vmem = pl.BlockSpec(memory_space=pltpu.VMEM)
    return pl.pallas_call(
        layers_kernel,
        out_shape=[
            jax.ShapeDtypeStruct((tokens, width), jnp.bfloat16),
            jax.ShapeDtypeStruct((1, 128), jnp.float32),
        ],
        in_specs=[pl.BlockSpec(memory_space=pltpu.SMEM), pl.BlockSpec(memory_space=pl.ANY)],
        out_specs=[vmem, vmem],
        scratch_shapes=scratch,
        compiler_params=pltpu.CompilerParams(collective_id=4, has_side_effects=True, vmem_limit_bytes=VMEM_LIMIT),
    )(own_len, product)


def per_device(hidden, rotation, norm_gain, value_weight, output_weight, lengths):
    tokens, width = hidden.shape
    layers, part = output_weight.shape[0], output_weight.shape[1]
    scaled = (norm_gain[:, :, None] * value_weight.astype(jnp.float32)).astype(jnp.bfloat16)
    own = jnp.concatenate([jnp.transpose(scaled, (0, 2, 1)), output_weight], axis=0)
    product = rotate(rotation, hidden, own.reshape(2 * layers * part, width))
    own_len = lax.dynamic_slice_in_dim(lengths, lax.axis_index(DP), 1)
    out, total = run_layers(own_len, product, tokens, part * lax.axis_size(DP), part)
    count = jnp.sum(lengths).astype(jnp.float32)
    return out, total[0, 0] / count


def solution(mesh):
    finer = Mesh(mesh.devices.reshape(4, 4, 4, 2), DP)
    in_specs = (P(DP, None), P(DP, None), P(), P(None, None, DP), P(None, DP, None), P())
    out_specs = (P(DP, None), P())
    return jax.shard_map(per_device, mesh=finer, in_specs=in_specs, out_specs=out_specs, check_vma=False)
```

```python
import functools

import jax
import jax.numpy as jnp
from jax import lax
from jax.experimental import pallas as pl
from jax.experimental.pallas import tpu as pltpu
from jax.sharding import Mesh
from jax.sharding import PartitionSpec as P

DP = ("dp_0", "dp_1", "dp_2", "dp_3")
EPS_NORM = 1e-06
EPS_SCALE = 1e-06
CLIP_RATIO = 0.9
SOFT = (6.579714691285096, -12.986868668454669, 12.191614515303863, -6.570949514891455, 1.970640660123473)
ROW_STEP = 256
SUB = 64
VMEM_LIMIT = 63 * 1024 * 1024
MESH_ID = pl.DeviceIdType.MESH


def soft_round(values):
    whole = jnp.round(values)
    rest = values - whole
    square = rest * rest
    poly = SOFT[4] * square + SOFT[3]
    for coefficient in (SOFT[2], SOFT[1], SOFT[0]):
        poly = poly * square + coefficient
    return whole + (rest * square) * poly


def fake_quant(values, step_size):
    return soft_round(jnp.clip(values / step_size, -8.0, 7.0)) * step_size


RING = 4
COLORS = ((0, 1, 2), (1, 2, 0), (2, 0, 1))


class Gather:
    def __init__(self, buffer, place, send, recv, first_row, rows, parts, first_column, widths):
        self.buffer, self.place, self.send, self.recv = buffer, place, send, recv
        self.half = buffer.shape[4] // 2
        self.first_row, self.rows, self.parts = first_row, rows, parts
        self.first_column, self.widths = first_column, widths
        self.partner = {DP[3]: 1 - place[3]}
        self.pending = {None: []}
        self.state = {}
        self.counter = 0

    def view(self, color, position, phase, part, side=None):
        order = COLORS[color]
        done = order[:phase]
        start = self.first_column + sum(self.widths[:color])
        cols = pl.ds(pl.multiple_of(self.place[3] * self.half + start, 128), self.widths[color])
        index = [self.place[k] for k in range(3)]
        for k in done:
            index[k] = slice(None)
        index[order[phase]] = position
        if side is not None:
            index[done[0]] = pl.ds(2 * side, 2)
        rows = pl.ds(self.first_row, self.rows)
        if part is not None:
            count = self.rows // self.parts
            rows = pl.ds(self.first_row + part * count, count)
        return self.buffer.at[index[0], index[1], index[2], rows, cols]

    def copy(self, view, peer, part):
        slot = self.counter
        self.counter += 1
        copy = pltpu.make_async_remote_copy(
            src_ref=view, dst_ref=view, send_sem=self.send.at[slot], recv_sem=self.recv.at[slot],
            device_id=peer, device_id_type=MESH_ID,
        )
        copy.start()
        self.pending.setdefault(part, []).append((copy, peer is self.partner))
        return copy

    def ring(self, color, phase):
        axis = COLORS[color][phase]
        own = self.place[axis]
        return axis, own, lax.rem(own + 1, RING), lax.rem(own + 2, RING), lax.rem(own + RING - 1, RING)

    def begin(self, phase, part=None):
        for color in range(3):
            axis, own, above, across, below = self.ring(color, phase)
            block = self.view(color, own, phase, part)
            copies = [self.copy(block, {DP[axis]: above}, part), self.copy(block, {DP[axis]: below}, part)]
            if phase == 0:
                copies.append(self.copy(block, {DP[axis]: across}, part))
            self.state[phase, color, part] = copies

    def relay(self, phase, part=None):
        for color in range(3):
            axis, own, above, across, below = self.ring(color, phase)
            from_below, from_above = self.state[phase, color, part]
            from_below.wait_recv()
            first = self.copy(self.view(color, below, phase, part, 0), {DP[axis]: above}, part)
            self.copy(self.view(color, below, phase, part), self.partner, part)
            from_above.wait_recv()
            second = self.copy(self.view(color, above, phase, part, 1), {DP[axis]: below}, part)
            self.copy(self.view(color, above, phase, part), self.partner, part)
            self.state[phase, color, part] = [first, second]

    def finish(self, phase, part=None):
        for color in range(3):
            axis, own, above, across, below = self.ring(color, phase)
            for copy in self.state[phase, color, part]:
                copy.wait_recv()
            self.copy(self.view(color, across, phase, part), self.partner, part)
            if phase == 0:
                self.copy(self.view(color, below, phase, part), self.partner, part)
                self.copy(self.view(color, above, phase, part), self.partner, part)

    def drain(self, part=None):
        for copy, kept in self.pending.pop(part, []):
            copy.wait_send()
            if kept:
                copy.wait_recv()


def gather_slots(parts):
    return 3 * (6 + 7 + 7 * parts)


NEAR = [(dy, dc) for dy in range(4) for dc in range(2) if (dy, dc) != (0, 0)]
FAR = [(dx, dz) for dx in range(4) for dz in range(4) if (dx, dz) != (0, 0)]


def near_peers(place):
    return [{DP[2]: lax.rem(place[2] + dy, 4), DP[3]: lax.rem(place[3] + dc, 2)} for dy, dc in NEAR]


def far_peers(place):
    return [{DP[0]: lax.rem(place[0] + dx, 4), DP[1]: lax.rem(place[1] + dz, 4)} for dx, dz in FAR]


class Exchange:
    def __init__(self, combine, place, buffers):
        self.combine, self.place = combine, place
        self.source, self.near, self.mid, self.far = buffers[:4]
        self.near_send, self.near_recv, self.far_send, self.far_recv = buffers[4:]

    def share(self, source, slots, me, peers, send, recv):
        slots[me] = source[...]
        copies = [
            pltpu.make_async_remote_copy(
                src_ref=source, dst_ref=slots.at[me], send_sem=send.at[k], recv_sem=recv.at[k],
                device_id=peer, device_id_type=MESH_ID,
            )
            for k, peer in enumerate(peers)
        ]
        for copy in copies:
            copy.start()
        return copies

    def total(self, slots, copies):
        for copy in copies:
            copy.wait()
        result = slots[0]
        for k in range(1, slots.shape[0]):
            result = self.combine(result, slots[k])
        return result

    def start(self, value):
        self.source[...] = value
        me = self.place[2] * 2 + self.place[3]
        self.copies = self.share(self.source, self.near, me, near_peers(self.place), self.near_send, self.near_recv)

    def turn(self):
        self.mid[...] = self.total(self.near, self.copies)
        me = self.place[0] * 4 + self.place[1]
        self.copies = self.share(self.mid, self.far, me, far_peers(self.place), self.far_send, self.far_recv)

    def finish(self):
        return self.total(self.far, self.copies)


def exchange_scratch(shape):
    return [
        pltpu.VMEM(shape, jnp.float32),
        pltpu.VMEM((8,) + shape, jnp.float32),
        pltpu.VMEM(shape, jnp.float32),
        pltpu.VMEM((16,) + shape, jnp.float32),
        pltpu.SemaphoreType.DMA((len(NEAR),)),
        pltpu.SemaphoreType.DMA((len(NEAR),)),
        pltpu.SemaphoreType.DMA((len(FAR),)),
        pltpu.SemaphoreType.DMA((len(FAR),)),
    ]


def quantize_rows(resid, act, square, error, first, count):
    width = resid.shape[1]

    def step(index, carry):
        rows = pl.ds(pl.multiple_of(first + index * SUB, SUB), SUB)
        squares = jnp.zeros((SUB, 128), jnp.float32)
        tops = jnp.zeros((SUB, 128), jnp.float32)
        for start in range(0, width, 128):
            part = resid[rows, start : start + 128]
            squares = squares + part * part
            tops = jnp.maximum(tops, jnp.abs(part))
        mean_sq = jnp.sum(squares, axis=1, keepdims=True) / width
        scale = lax.rsqrt(mean_sq + EPS_NORM)
        step_size = CLIP_RATIO * (jnp.max(tops, axis=1, keepdims=True) * scale) / 7.0 + EPS_SCALE
        gain = jnp.broadcast_to(scale / step_size, (SUB, 128))
        wide_step = jnp.broadcast_to(step_size, (SUB, 128))
        errors = jnp.zeros((SUB, 128), jnp.float32)
        for start in range(0, width, 128):
            units = resid[rows, start : start + 128] * gain
            rounded = soft_round(jnp.minimum(jnp.maximum(units, -8.0), 7.0))
            gap = rounded - units
            errors = errors + gap * gap
            act[rows, start : start + 128] = (rounded * wide_step).astype(jnp.bfloat16)
        square[rows, :] = mean_sq
        error[rows, :] = jnp.sum(errors, axis=1, keepdims=True) * (step_size * step_size)
        return carry

    lax.fori_loop(0, count // SUB, step, 0)


def quantize_mixed(mixed, gain, step_size, mix, error, first, count):
    channels = mixed.shape[1]

    def step(index, carry):
        rows = pl.ds(pl.multiple_of(first + index * SUB, SUB), SUB)
        errors = jnp.zeros((SUB, 128), jnp.float32)
        for start in range(0, channels, 128):
            cols = slice(start, start + 128)
            units = mixed[rows, cols] * gain[:, cols]
            rounded = soft_round(jnp.minimum(jnp.maximum(units, -8.0), 7.0))
            gap = (rounded - units) * step_size[:, cols]
            errors = errors + gap * gap
            mix[rows, cols] = (rounded * step_size[:, cols]).astype(jnp.bfloat16)
        error[rows, :] = jnp.sum(errors, axis=1, keepdims=True)
        return carry

    lax.fori_loop(0, count // SUB, step, 0)


def window_kernel(
    len_ref, all_len_ref, rotation_ref, value_ref, norm_ref, weight_ref, hidden_ref, out_ref, sum_ref,
    turn, full, product, left, mixed, mix, pair, wide, square, error, loss, top, gain, step_size,
    turn_send, turn_recv, ring_send, ring_recv, swap_send, swap_recv, local, *exchanges,
):
    place = [lax.axis_index(name) for name in DP]
    core = place[3]
    own_len = len_ref[((place[0] * RING + place[1]) * RING + place[2]) * 2 + core]
    tokens, width = hidden_ref.shape
    channels = mixed.shape[1]
    part = weight_ref.shape[1]
    shard = rotation_ref.shape[0]
    act = left
    barrier = pltpu.get_barrier_semaphore()
    peers = near_peers(place) + far_peers(place)
    for peer in peers:
        pl.semaphore_signal(barrier, inc=1, device_id=peer, device_id_type=MESH_ID)
    load = pltpu.make_async_copy(hidden_ref, left.at[pl.ds(0, tokens)], local.at[0])
    load.start()
    tops_max = Exchange(jnp.maximum, place, exchanges[0:8])
    ranges = [Exchange(jnp.maximum, place, exchanges[8:16]), Exchange(jnp.maximum, place, exchanges[16:24])]
    loss_sum = Exchange(jnp.add, place, exchanges[24:32])

    def swap(source, target, slot):
        copy = pltpu.make_async_remote_copy(
            src_ref=source, dst_ref=target, send_sem=swap_send.at[slot], recv_sem=swap_recv.at[slot],
            device_id={DP[3]: 1 - core}, device_id_type=MESH_ID,
        )
        copy.start()
        return copy

    both_shards = wide
    both_shards[core] = rotation_ref[...]
    small = [
        (norm_ref[k : k + 1, :] * value_ref[k].astype(jnp.float32)).astype(jnp.bfloat16).astype(jnp.float32)
        for k in range(2)
    ] + [weight_ref[k].astype(jnp.float32) for k in range(2)]
    left[tokens : tokens + 4 * part, :] = jnp.concatenate(small, axis=0).astype(jnp.bfloat16)
    pl.semaphore_wait(barrier, len(peers))
    swapped = swap(rotation_ref, both_shards.at[core], 0)
    swapped.wait()
    turn[place[0], place[1], place[2]] = jnp.concatenate(
        [both_shards[0].astype(jnp.float32), both_shards[1].astype(jnp.float32)], axis=0
    ).astype(jnp.bfloat16)
    early = Gather(turn, place, turn_send.at[0], turn_recv.at[0], 0, 2 * shard, 1, 0, (256, 256, 256))
    late = Gather(turn, place, turn_send.at[1], turn_recv.at[1], 0, 2 * shard, 1, 768, (256, 128, 128))
    chunk = 256

    def columns(first_row, rows, first, count):
        def body(index, carry):
            for core_half in range(2):
                cols = pl.ds(pl.multiple_of(core_half * (width // 2) + first + index * chunk, chunk), chunk)
                block = turn[:, :, :, :, cols].reshape(width, chunk)
                product[first_row : first_row + rows, cols] = jnp.dot(
                    left[first_row : first_row + rows, :], block, preferred_element_type=jnp.float32
                )
            return carry

        lax.fori_loop(0, count, body, 0)

    early.begin(0)
    late.begin(0)
    early.finish(0)
    early.begin(1)
    late.finish(0)
    late.begin(1)
    early.relay(1)
    late.relay(1)
    early.finish(1)
    early.begin(2)
    load.wait()
    early.relay(2)
    late.finish(1)
    late.begin(2)
    early.finish(2)
    early.drain()
    late.relay(2)
    columns(0, tokens + 4 * part, 0, 3)
    late.finish(2)
    late.drain()
    columns(tokens, 4 * part, 768, 2)

    def matrix(which):
        return product[tokens + which * part : tokens + (which + 1) * part, :]

    def combine(first):
        for k in (first, first + 1):
            both = jnp.concatenate([pair[0, k].astype(jnp.float32), pair[1, k].astype(jnp.float32)], axis=0)
            full[place[0], place[1], place[2], 2 * part * k : 2 * part * (k + 1), :] = both.astype(jnp.bfloat16)

    def weights(which):
        return full[:, :, :, 2 * part * which : 2 * part * (which + 1), :].reshape(channels, width)

    done = 0

    def rows_ahead(count):
        nonlocal done
        quantize_rows(product, act, square, error, done, count)
        done = done + count

    for k in range(2):
        value = matrix(k)
        value_top = jnp.max(jnp.abs(value), axis=1, keepdims=True)
        pair[core, k] = fake_quant(value, value_top / 7.0 + EPS_SCALE).astype(jnp.bfloat16)
    output_tops = jnp.concatenate(
        [jnp.max(jnp.abs(matrix(k)), axis=0, keepdims=True) for k in (2, 3)], axis=0
    )
    spot = pair.at[core, pl.ds(0, 2)]
    swapped = swap(spot, spot, 1)
    tops_max.start(output_tops)
    values = Gather(full, place, ring_send.at[0], ring_recv.at[0], 0, 4 * part, 2, 0, (512, 384, 384))
    outputs = Gather(full, place, ring_send.at[1], ring_recv.at[1], 4 * part, 4 * part, 2, 0, (384, 512, 384))
    swapped.wait()
    combine(0)
    values.begin(0)
    columns(0, tokens, 768, 1)
    values.finish(0)
    values.begin(1)
    tops_max.turn()
    columns(0, tokens, 1024, 1)
    values.relay(1)
    rows_ahead(64)
    tops = tops_max.finish()
    for k in (2, 3):
        size = tops[k - 2 : k - 1, :] / 7.0 + EPS_SCALE
        pair[core, k] = fake_quant(matrix(k), size).astype(jnp.bfloat16)
    spot = pair.at[core, pl.ds(2, 2)]
    swapped = swap(spot, spot, 2)
    values.finish(1)
    values.begin(2, 0)
    swapped.wait()
    combine(2)
    outputs.begin(0)
    rows_ahead(192)
    values.relay(2, 0)
    outputs.finish(0)
    outputs.begin(1)
    values.begin(2, 1)
    rows_ahead(256)
    values.finish(2, 0)
    outputs.relay(1)
    rows_ahead(256)
    values.relay(2, 1)
    outputs.finish(1)
    outputs.begin(2, 0)
    outputs.begin(2, 1)
    values.drain()
    values.drain(0)

    def live_rows(first, count):
        return first + lax.broadcasted_iota(jnp.int32, (count, 1), 0) < own_len

    def mix_block(first, which):
        rows = pl.ds(pl.multiple_of(first, ROW_STEP), ROW_STEP)
        block = lax.dot_general(
            act[rows, :], weights(which), (((1,), (1,)), ((), ())), preferred_element_type=jnp.float32
        )
        mixed[rows, :] = block
        seen = jnp.where(live_rows(first, ROW_STEP), jnp.abs(block), 0.0)
        top[...] = jnp.maximum(top[...], jnp.max(seen.reshape(ROW_STEP // 8, 8, channels), axis=0))

    def set_steps(vrange):
        sizes = CLIP_RATIO * vrange / 7.0 + EPS_SCALE
        step_size[...] = sizes
        gain[...] = 1.0 / sizes

    top[...] = jnp.zeros_like(top)
    loss[...] = square[...] * error[...]
    blocks = tokens // ROW_STEP

    def first(index, carry):
        mix_block(index * ROW_STEP, 0)
        return carry

    lax.fori_loop(0, blocks, first, 0)
    ranges[0].start(jnp.max(top[...], axis=0, keepdims=True))
    values.finish(2, 1)
    outputs.relay(2, 0)
    ranges[0].turn()
    outputs.relay(2, 1)
    outputs.finish(2, 0)
    set_steps(ranges[0].finish())
    values.drain(1)
    outputs.drain()
    outputs.drain(0)
    top[...] = jnp.zeros_like(top)

    def middle(index, carry):
        first = index * ROW_STEP
        rows = pl.ds(pl.multiple_of(first, ROW_STEP), ROW_STEP)
        quantize_mixed(mixed, gain, step_size, mix, error, first, ROW_STEP)
        loss[rows, :] = loss[rows, :] + square[rows, :] * error[rows, :]
        product[rows, :] = product[rows, :] + jnp.dot(mix[rows, :], weights(2), preferred_element_type=jnp.float32)
        quantize_rows(product, act, square, error, first, ROW_STEP)
        loss[rows, :] = loss[rows, :] + square[rows, :] * error[rows, :]
        mix_block(first, 1)
        return carry

    lax.fori_loop(0, 1, middle, 0)
    outputs.finish(2, 1)
    lax.fori_loop(1, blocks, middle, 0)
    ranges[1].start(jnp.max(top[...], axis=0, keepdims=True))
    outputs.drain(1)
    ranges[1].turn()
    set_steps(ranges[1].finish())
    quantize_mixed(mixed, gain, step_size, mix, error, 0, tokens)
    kept = jnp.where(live_rows(0, tokens), loss[...] + square[...] * error[...], 0.0)
    loss_sum.start(jnp.broadcast_to(jnp.sum(kept, axis=0, keepdims=True), sum_ref.shape))

    def store(index):
        rows = pl.ds(pl.multiple_of(index * ROW_STEP, ROW_STEP), ROW_STEP)
        return pltpu.make_async_copy(act.at[rows], out_ref.at[rows], local.at[1 + index])

    def last(index, carry):
        first = index * ROW_STEP
        rows = pl.ds(pl.multiple_of(first, ROW_STEP), ROW_STEP)
        updated = product[rows, :] + jnp.dot(mix[rows, :], weights(3), preferred_element_type=jnp.float32)
        act[rows, :] = jnp.where(live_rows(first, ROW_STEP), updated, 0.0).astype(jnp.bfloat16)
        store(index).start()
        return carry

    lax.fori_loop(0, 1, last, 0)
    loss_sum.turn()
    lax.fori_loop(1, blocks, last, 0)
    count = jnp.sum(all_len_ref[...].astype(jnp.float32), axis=1, keepdims=True)
    sum_ref[...] = loss_sum.finish() / count
    for index in range(blocks):
        store(index).wait()


def per_device(hidden, rotation, norm_gain, value_weight, output_weight, lengths):
    tokens, width = hidden.shape
    layers, part = output_weight.shape[0], output_weight.shape[1]
    channels = part * lax.axis_size(DP)
    shard = rotation.shape[0]
    column = pltpu.VMEM((tokens, 1), jnp.float32)
    cube = (RING, RING, RING)
    dma = pltpu.SemaphoreType.DMA
    scratch = [
        pltpu.VMEM(cube + (2 * shard, width), jnp.bfloat16),
        pltpu.VMEM(cube + (4 * layers * part, width), jnp.bfloat16),
        pltpu.VMEM((tokens + 2 * layers * part, width), jnp.float32),
        pltpu.VMEM((tokens + 2 * layers * part, width), jnp.bfloat16),
        pltpu.VMEM((tokens, channels), jnp.float32),
        pltpu.VMEM((tokens, channels), jnp.bfloat16),
        pltpu.VMEM((2, 2 * layers, part, width), jnp.bfloat16),
        pltpu.VMEM((2, shard, width), jnp.bfloat16),
        column, column, column,
        pltpu.VMEM((8, channels), jnp.float32),
        pltpu.VMEM((1, channels), jnp.float32),
        pltpu.VMEM((1, channels), jnp.float32),
        dma((2, gather_slots(1))), dma((2, gather_slots(1))),
        dma((2, gather_slots(2))), dma((2, gather_slots(2))),
        dma((3,)), dma((3,)), dma((1 + tokens // ROW_STEP,)),
    ]
    for shape in ((layers, width), (1, channels), (1, channels), (1, 128)):
        scratch = scratch + exchange_scratch(shape)
    vmem = pl.BlockSpec(memory_space=pltpu.VMEM)
    out, total = pl.pallas_call(
        window_kernel,
        out_shape=[
            jax.ShapeDtypeStruct((tokens, width), jnp.bfloat16),
            jax.ShapeDtypeStruct((1, 128), jnp.float32),
        ],
        in_specs=[pl.BlockSpec(memory_space=pltpu.SMEM)] + [vmem] * 5 + [pl.BlockSpec(memory_space=pl.ANY)],
        out_specs=[pl.BlockSpec(memory_space=pl.ANY), vmem],
        scratch_shapes=scratch,
        compiler_params=pltpu.CompilerParams(collective_id=4, has_side_effects=True, vmem_limit_bytes=VMEM_LIMIT),
    )(
        lengths, lengths.reshape(1, -1), rotation, jnp.transpose(value_weight, (0, 2, 1)), norm_gain,
        output_weight, hidden,
    )
    return out, total[0, 0]


def solution(mesh):
    finer = Mesh(mesh.devices.reshape(4, 4, 4, 2), DP)
    in_specs = (P(DP, None), P(DP, None), P(), P(None, None, DP), P(None, DP, None), P())
    out_specs = (P(DP, None), P())
    return jax.shard_map(per_device, mesh=finer, in_specs=in_specs, out_specs=out_specs, check_vma=False)
```

```python
import functools

import jax
import jax.numpy as jnp
from jax import lax
from jax.experimental import pallas as pl
from jax.experimental.pallas import tpu as pltpu
from jax.sharding import Mesh
from jax.sharding import PartitionSpec as P

DP = ("dp_0", "dp_1", "dp_2", "dp_3")
EPS_NORM = 1e-06
EPS_SCALE = 1e-06
CLIP_RATIO = 0.9
SOFT = (6.579714691285096, -12.986868668454669, 12.191614515303863, -6.570949514891455, 1.970640660123473)
ROW_STEP = 256
SUB = 64
VMEM_LIMIT = 58 * 1024 * 1024
MESH_ID = pl.DeviceIdType.MESH


def soft_round(values):
    whole = jnp.round(values)
    rest = values - whole
    square = rest * rest
    poly = SOFT[4] * square + SOFT[3]
    for coefficient in (SOFT[2], SOFT[1], SOFT[0]):
        poly = poly * square + coefficient
    return whole + (rest * square) * poly


def fake_quant(values, step_size):
    return soft_round(jnp.clip(values / step_size, -8.0, 7.0)) * step_size


RING = 4
COLORS = ((0, 1, 2), (1, 2, 0), (2, 0, 1))


class Gather:
    def __init__(self, buffer, place, send, recv, areas, parts):
        self.buffer, self.place, self.send, self.recv = buffer, place, send, recv
        self.half = buffer.shape[4] // 2
        self.areas, self.parts = areas, parts
        self.partner = {DP[3]: 1 - place[3]}
        self.pending = {None: []}
        self.state = {}
        self.counter = 0

    def view(self, color, position, phase, part, side=None):
        which, first_row, count, start, width = self.areas[color]
        order = COLORS[which]
        done = order[:phase]
        cols = pl.ds(pl.multiple_of(self.place[3] * self.half + start, 128), width)
        index = [self.place[k] for k in range(3)]
        for k in done:
            index[k] = slice(None)
        index[order[phase]] = position
        if side is not None:
            index[done[0]] = pl.ds(2 * side, 2)
        rows = pl.ds(first_row, count)
        if part is not None:
            count = count // self.parts
            rows = pl.ds(first_row + part * count, count)
        return self.buffer.at[index[0], index[1], index[2], rows, cols]

    def copy(self, view, peer, part):
        slot = self.counter
        self.counter += 1
        copy = pltpu.make_async_remote_copy(
            src_ref=view, dst_ref=view, send_sem=self.send.at[slot], recv_sem=self.recv.at[slot],
            device_id=peer, device_id_type=MESH_ID,
        )
        copy.start()
        self.pending.setdefault(part, []).append((copy, peer is self.partner))
        return copy

    def ring(self, color, phase):
        axis = COLORS[self.areas[color][0]][phase]
        own = self.place[axis]
        return axis, own, lax.rem(own + 1, RING), lax.rem(own + 2, RING), lax.rem(own + RING - 1, RING)

    def begin(self, phase, part=None):
        for color in range(len(self.areas)):
            axis, own, above, across, below = self.ring(color, phase)
            block = self.view(color, own, phase, part)
            copies = [self.copy(block, {DP[axis]: above}, part), self.copy(block, {DP[axis]: below}, part)]
            if phase == 0:
                copies.append(self.copy(block, {DP[axis]: across}, part))
            self.state[phase, color, part] = copies

    def relay(self, phase, part=None):
        for color in range(len(self.areas)):
            axis, own, above, across, below = self.ring(color, phase)
            from_below, from_above = self.state[phase, color, part]
            from_below.wait_recv()
            first = self.copy(self.view(color, below, phase, part, 0), {DP[axis]: above}, part)
            self.copy(self.view(color, below, phase, part), self.partner, part)
            from_above.wait_recv()
            second = self.copy(self.view(color, above, phase, part, 1), {DP[axis]: below}, part)
            self.copy(self.view(color, above, phase, part), self.partner, part)
            self.state[phase, color, part] = [first, second]

    def finish(self, phase, part=None):
        for color in range(len(self.areas)):
            axis, own, above, across, below = self.ring(color, phase)
            for copy in self.state[phase, color, part]:
                copy.wait_recv()
            self.copy(self.view(color, across, phase, part), self.partner, part)
            if phase == 0:
                self.copy(self.view(color, below, phase, part), self.partner, part)
                self.copy(self.view(color, above, phase, part), self.partner, part)

    def drain(self, part=None):
        for copy, kept in self.pending.pop(part, []):
            copy.wait_send()
            if kept:
                copy.wait_recv()


def bands(first_row, rows, first_column, widths):
    return [
        (k, first_row, rows, first_column + sum(widths[:k]), width) for k, width in enumerate(widths)
    ]


def gather_slots(areas, parts):
    return areas * (6 + 7 + 7 * parts)


NEAR = [(dy, dc) for dy in range(4) for dc in range(2) if (dy, dc) != (0, 0)]
FAR = [(dx, dz) for dx in range(4) for dz in range(4) if (dx, dz) != (0, 0)]


def near_peers(place):
    return [{DP[2]: lax.rem(place[2] + dy, 4), DP[3]: lax.rem(place[3] + dc, 2)} for dy, dc in NEAR]


def far_peers(place):
    return [{DP[0]: lax.rem(place[0] + dx, 4), DP[1]: lax.rem(place[1] + dz, 4)} for dx, dz in FAR]


class Exchange:
    def __init__(self, combine, place, buffers):
        self.combine, self.place = combine, place
        self.source, self.near, self.mid, self.far = buffers[:4]
        self.near_send, self.near_recv, self.far_send, self.far_recv = buffers[4:]

    def share(self, source, slots, me, peers, send, recv):
        slots[me] = source[...]
        copies = [
            pltpu.make_async_remote_copy(
                src_ref=source, dst_ref=slots.at[me], send_sem=send.at[k], recv_sem=recv.at[k],
                device_id=peer, device_id_type=MESH_ID,
            )
            for k, peer in enumerate(peers)
        ]
        for copy in copies:
            copy.start()
        return copies

    def total(self, slots, copies):
        for copy in copies:
            copy.wait()
        result = slots[0]
        for k in range(1, slots.shape[0]):
            result = self.combine(result, slots[k])
        return result

    def start(self, value):
        self.source[...] = value
        me = self.place[2] * 2 + self.place[3]
        self.copies = self.share(self.source, self.near, me, near_peers(self.place), self.near_send, self.near_recv)

    def turn(self):
        self.mid[...] = self.total(self.near, self.copies)
        me = self.place[0] * 4 + self.place[1]
        self.copies = self.share(self.mid, self.far, me, far_peers(self.place), self.far_send, self.far_recv)

    def finish(self):
        return self.total(self.far, self.copies)


def exchange_scratch(shape):
    return [
        pltpu.VMEM(shape, jnp.float32),
        pltpu.VMEM((8,) + shape, jnp.float32),
        pltpu.VMEM(shape, jnp.float32),
        pltpu.VMEM((16,) + shape, jnp.float32),
        pltpu.SemaphoreType.DMA((len(NEAR),)),
        pltpu.SemaphoreType.DMA((len(NEAR),)),
        pltpu.SemaphoreType.DMA((len(FAR),)),
        pltpu.SemaphoreType.DMA((len(FAR),)),
    ]


def quantize_rows(resid, act, square, error, first, count, sub=SUB):
    width = resid.shape[1]

    def step(index, carry):
        rows = pl.ds(pl.multiple_of(first + index * sub, sub), sub)
        squares = jnp.zeros((sub, 128), jnp.float32)
        tops = jnp.zeros((sub, 128), jnp.float32)
        for start in range(0, width, 128):
            part = resid[rows, start : start + 128]
            squares = squares + part * part
            tops = jnp.maximum(tops, jnp.abs(part))
        mean_sq = jnp.sum(squares, axis=1, keepdims=True) / width
        scale = lax.rsqrt(mean_sq + EPS_NORM)
        step_size = CLIP_RATIO * (jnp.max(tops, axis=1, keepdims=True) * scale) / 7.0 + EPS_SCALE
        gain = jnp.broadcast_to(scale / step_size, (sub, 128))
        wide_step = jnp.broadcast_to(step_size, (sub, 128))
        errors = jnp.zeros((sub, 128), jnp.float32)
        for start in range(0, width, 128):
            units = resid[rows, start : start + 128] * gain
            rounded = soft_round(jnp.minimum(jnp.maximum(units, -8.0), 7.0))
            gap = rounded - units
            errors = errors + gap * gap
            act[rows, start : start + 128] = (rounded * wide_step).astype(jnp.bfloat16)
        square[rows, :] = mean_sq
        error[rows, :] = jnp.sum(errors, axis=1, keepdims=True) * (step_size * step_size)
        return carry

    lax.fori_loop(0, count // sub, step, 0)


def quantize_mixed(mixed, gain, step_size, mix, error, first, count, sub=SUB):
    channels = mixed.shape[1]

    def step(index, carry):
        rows = pl.ds(pl.multiple_of(first + index * sub, sub), sub)
        errors = jnp.zeros((sub, 128), jnp.float32)
        for start in range(0, channels, 128):
            cols = slice(start, start + 128)
            units = mixed[rows, cols] * gain[:, cols]
            rounded = soft_round(jnp.minimum(jnp.maximum(units, -8.0), 7.0))
            gap = (rounded - units) * step_size[:, cols]
            errors = errors + gap * gap
            mix[rows, cols] = (rounded * step_size[:, cols]).astype(jnp.bfloat16)
        error[rows, :] = jnp.sum(errors, axis=1, keepdims=True)
        return carry

    lax.fori_loop(0, count // sub, step, 0)


def window_kernel(
    len_ref, all_len_ref, rotation_ref, value_ref, norm_ref, weight_ref, hidden_ref, out_ref, sum_ref,
    turn, full, product, left, mixed, mix, pair, wide, square, error, loss, top, gain, step_size,
    turn_send, turn_recv, ring_send, ring_recv, swap_send, swap_recv, local, *exchanges,
):
    place = [lax.axis_index(name) for name in DP]
    core = place[3]
    own_len = len_ref[((place[0] * RING + place[1]) * RING + place[2]) * 2 + core]
    tokens, width = hidden_ref.shape
    channels = mixed.shape[1]
    part = weight_ref.shape[1]
    shard = rotation_ref.shape[0]
    act = left
    barrier = pltpu.get_barrier_semaphore()
    peers = near_peers(place) + far_peers(place)
    for peer in peers:
        pl.semaphore_signal(barrier, inc=1, device_id=peer, device_id_type=MESH_ID)
    load = pltpu.make_async_copy(hidden_ref, left.at[pl.ds(0, tokens)], local.at[0])
    load.start()
    tops_max = Exchange(jnp.maximum, place, exchanges[0:8])
    ranges = [Exchange(jnp.maximum, place, exchanges[8:16]), Exchange(jnp.maximum, place, exchanges[16:24])]
    loss_sum = Exchange(jnp.add, place, exchanges[24:32])

    def swap(source, target, slot):
        copy = pltpu.make_async_remote_copy(
            src_ref=source, dst_ref=target, send_sem=swap_send.at[slot], recv_sem=swap_recv.at[slot],
            device_id={DP[3]: 1 - core}, device_id_type=MESH_ID,
        )
        copy.start()
        return copy

    both_shards = wide
    both_shards[core] = rotation_ref[...]
    small = [
        (norm_ref[k : k + 1, :] * value_ref[k].astype(jnp.float32)).astype(jnp.bfloat16).astype(jnp.float32)
        for k in range(2)
    ] + [weight_ref[k].astype(jnp.float32) for k in range(2)]
    left[tokens : tokens + 4 * part, :] = jnp.concatenate(small, axis=0).astype(jnp.bfloat16)
    pl.semaphore_wait(barrier, len(peers))
    swapped = swap(rotation_ref, both_shards.at[core], 0)
    swapped.wait()
    turn[place[0], place[1], place[2]] = jnp.concatenate(
        [both_shards[0].astype(jnp.float32), both_shards[1].astype(jnp.float32)], axis=0
    ).astype(jnp.bfloat16)
    early = Gather(turn, place, turn_send.at[0], turn_recv.at[0], bands(0, 2 * shard, 0, (256, 256, 256)), 1)
    third = (2 * shard // 3 + 7) // 8 * 8
    slices = [(0, 0, third), (1, third, third), (2, 2 * third, 2 * shard - 2 * third)]
    shared = [(which, row, rows, 1152, 128) for which, row, rows in slices]
    late = Gather(
        turn, place, turn_send.at[1], turn_recv.at[1], bands(0, 2 * shard, 768, (128, 128, 128)) + shared, 1
    )
    chunk = 256

    def columns(first_row, rows, first, count):
        def body(index, carry):
            for core_half in range(2):
                cols = pl.ds(pl.multiple_of(core_half * (width // 2) + first + index * chunk, chunk), chunk)
                block = turn[:, :, :, :, cols].reshape(width, chunk)
                product[first_row : first_row + rows, cols] = jnp.dot(
                    left[first_row : first_row + rows, :], block, preferred_element_type=jnp.float32
                )
            return carry

        lax.fori_loop(0, count, body, 0)

    early.begin(0)
    late.begin(0)
    early.finish(0)
    early.begin(1)
    late.finish(0)
    late.begin(1)
    early.relay(1)
    late.relay(1)
    early.finish(1)
    early.begin(2)
    load.wait()
    early.relay(2)
    late.finish(1)
    late.begin(2)
    early.finish(2)
    early.drain()
    late.relay(2)
    columns(0, tokens + 4 * part, 0, 2)
    late.finish(2)
    columns(0, tokens + 4 * part, 512, 1)
    late.drain()
    columns(tokens, 4 * part, 768, 2)

    def matrix(which):
        return product[tokens + which * part : tokens + (which + 1) * part, :]

    def combine(first):
        for k in (first, first + 1):
            both = jnp.concatenate([pair[0, k].astype(jnp.float32), pair[1, k].astype(jnp.float32)], axis=0)
            full[place[0], place[1], place[2], 2 * part * k : 2 * part * (k + 1), :] = both.astype(jnp.bfloat16)

    def weights(which):
        return full[:, :, :, 2 * part * which : 2 * part * (which + 1), :].reshape(channels, width)

    done = 0

    def rows_ahead(count):
        nonlocal done
        quantize_rows(product, act, square, error, done, count)
        done = done + count

    for k in range(2):
        value = matrix(k)
        value_top = jnp.max(jnp.abs(value), axis=1, keepdims=True)
        pair[core, k] = fake_quant(value, value_top / 7.0 + EPS_SCALE).astype(jnp.bfloat16)
    output_tops = jnp.concatenate(
        [jnp.max(jnp.abs(matrix(k)), axis=0, keepdims=True) for k in (2, 3)], axis=0
    )
    spot = pair.at[core, pl.ds(0, 2)]
    swapped = swap(spot, spot, 1)
    tops_max.start(output_tops)
    wide_first, wide_second = (512, 384, 384), (384, 512, 384)
    values = Gather(full, place, ring_send.at[0], ring_recv.at[0], bands(0, 4 * part, 0, wide_first), 2)
    outputs = Gather(full, place, ring_send.at[1], ring_recv.at[1], bands(4 * part, 4 * part, 0, wide_second), 2)
    swapped.wait()
    combine(0)
    values.begin(0)
    columns(0, tokens, 768, 1)
    values.finish(0)
    values.begin(1)
    tops_max.turn()
    columns(0, tokens, 1024, 1)
    values.relay(1)
    rows_ahead(64)
    tops = tops_max.finish()
    for k in (2, 3):
        size = tops[k - 2 : k - 1, :] / 7.0 + EPS_SCALE
        pair[core, k] = fake_quant(matrix(k), size).astype(jnp.bfloat16)
    spot = pair.at[core, pl.ds(2, 2)]
    swapped = swap(spot, spot, 2)
    values.finish(1)
    swapped.wait()
    combine(2)
    outputs.begin(0)
    values.begin(2, 0)
    rows_ahead(192)
    outputs.finish(0)
    outputs.begin(1)
    rows_ahead(192)
    values.relay(2, 0)
    rows_ahead(64)
    outputs.relay(1)
    values.begin(2, 1)
    rows_ahead(256)
    values.finish(2, 0)
    outputs.finish(1)
    outputs.begin(2, 0)
    values.drain()
    values.drain(0)

    def live_rows(first, count):
        return first + lax.broadcasted_iota(jnp.int32, (count, 1), 0) < own_len

    def mix_block(first, which):
        rows = pl.ds(pl.multiple_of(first, ROW_STEP), ROW_STEP)
        block = lax.dot_general(
            act[rows, :], weights(which), (((1,), (1,)), ((), ())), preferred_element_type=jnp.float32
        )
        mixed[rows, :] = block
        seen = jnp.where(live_rows(first, ROW_STEP), jnp.abs(block), 0.0)
        top[...] = jnp.maximum(top[...], jnp.max(seen.reshape(ROW_STEP // 8, 8, channels), axis=0))

    def set_steps(vrange):
        sizes = CLIP_RATIO * vrange / 7.0 + EPS_SCALE
        step_size[...] = sizes
        gain[...] = 1.0 / sizes

    top[...] = jnp.zeros_like(top)
    loss[...] = square[...] * error[...]
    blocks = tokens // ROW_STEP

    def first(index, carry):
        mix_block(index * ROW_STEP, 0)
        return carry

    lax.fori_loop(0, blocks - 1, first, 0)
    values.relay(2, 1)
    lax.fori_loop(blocks - 1, blocks, first, 0)
    ranges[0].start(jnp.max(top[...], axis=0, keepdims=True))
    ranges[0].turn()
    outputs.relay(2, 0)
    values.finish(2, 1)
    outputs.begin(2, 1)
    outputs.finish(2, 0)
    set_steps(ranges[0].finish())
    values.drain(1)
    outputs.drain()
    outputs.drain(0)
    top[...] = jnp.zeros_like(top)

    def middle(index, carry):
        first = index * ROW_STEP
        rows = pl.ds(pl.multiple_of(first, ROW_STEP), ROW_STEP)
        quantize_mixed(mixed, gain, step_size, mix, error, first, ROW_STEP, 128)
        loss[rows, :] = loss[rows, :] + square[rows, :] * error[rows, :]
        product[rows, :] = product[rows, :] + jnp.dot(mix[rows, :], weights(2), preferred_element_type=jnp.float32)
        quantize_rows(product, act, square, error, first, ROW_STEP, 128)
        loss[rows, :] = loss[rows, :] + square[rows, :] * error[rows, :]
        mix_block(first, 1)
        return carry

    lax.fori_loop(0, 1, middle, 0)
    outputs.relay(2, 1)
    lax.fori_loop(1, blocks, middle, 0)
    outputs.finish(2, 1)
    ranges[1].start(jnp.max(top[...], axis=0, keepdims=True))
    outputs.drain(1)
    ranges[1].turn()
    set_steps(ranges[1].finish())
    quantize_mixed(mixed, gain, step_size, mix, error, 0, tokens, 128)
    kept = jnp.where(live_rows(0, tokens), loss[...] + square[...] * error[...], 0.0)
    loss_sum.start(jnp.broadcast_to(jnp.sum(kept, axis=0, keepdims=True), sum_ref.shape))

    def last(index, carry):
        first = index * ROW_STEP
        rows = pl.ds(pl.multiple_of(first, ROW_STEP), ROW_STEP)
        updated = product[rows, :] + jnp.dot(mix[rows, :], weights(3), preferred_element_type=jnp.float32)
        out_ref[rows, :] = jnp.where(live_rows(first, ROW_STEP), updated, 0.0).astype(jnp.bfloat16)
        return carry

    lax.fori_loop(0, 1, last, 0)
    loss_sum.turn()
    lax.fori_loop(1, blocks, last, 0)
    count = jnp.sum(all_len_ref[...].astype(jnp.float32), axis=1, keepdims=True)
    sum_ref[...] = loss_sum.finish() / count


def per_device(hidden, rotation, norm_gain, value_weight, output_weight, lengths):
    tokens, width = hidden.shape
    layers, part = output_weight.shape[0], output_weight.shape[1]
    channels = part * lax.axis_size(DP)
    shard = rotation.shape[0]
    column = pltpu.VMEM((tokens, 1), jnp.float32)
    cube = (RING, RING, RING)
    dma = pltpu.SemaphoreType.DMA
    scratch = [
        pltpu.VMEM(cube + (2 * shard, width), jnp.bfloat16),
        pltpu.VMEM(cube + (4 * layers * part, width), jnp.bfloat16),
        pltpu.VMEM((tokens + 2 * layers * part, width), jnp.float32),
        pltpu.VMEM((tokens + 2 * layers * part, width), jnp.bfloat16),
        pltpu.VMEM((tokens, channels), jnp.float32),
        pltpu.VMEM((tokens, channels), jnp.bfloat16),
        pltpu.VMEM((2, 2 * layers, part, width), jnp.bfloat16),
        pltpu.VMEM((2, shard, width), jnp.bfloat16),
        column, column, column,
        pltpu.VMEM((8, channels), jnp.float32),
        pltpu.VMEM((1, channels), jnp.float32),
        pltpu.VMEM((1, channels), jnp.float32),
        dma((2, gather_slots(6, 1))), dma((2, gather_slots(6, 1))),
        dma((2, gather_slots(3, 2))), dma((2, gather_slots(3, 2))),
        dma((3,)), dma((3,)), dma((1,)),
    ]
    for shape in ((layers, width), (1, channels), (1, channels), (1, 128)):
        scratch = scratch + exchange_scratch(shape)
    vmem = pl.BlockSpec(memory_space=pltpu.VMEM)
    out, total = pl.pallas_call(
        window_kernel,
        out_shape=[
            pltpu.VMEM((tokens, width), jnp.bfloat16),
            pltpu.VMEM((1, 128), jnp.float32),
        ],
        in_specs=[pl.BlockSpec(memory_space=pltpu.SMEM)] + [vmem] * 5 + [pl.BlockSpec(memory_space=pl.ANY)],
        out_specs=[vmem, vmem],
        scratch_shapes=scratch,
        compiler_params=pltpu.CompilerParams(collective_id=4, has_side_effects=True, vmem_limit_bytes=VMEM_LIMIT),
    )(
        lengths, lengths.reshape(1, -1), rotation, jnp.transpose(value_weight, (0, 2, 1)), norm_gain,
        output_weight, hidden,
    )
    return out, total[0, 0]


def solution(mesh):
    finer = Mesh(mesh.devices.reshape(4, 4, 4, 2), DP)
    in_specs = (P(DP, None), P(DP, None), P(), P(None, None, DP), P(None, DP, None), P())
    out_specs = (P(DP, None), P())
    return jax.shard_map(per_device, mesh=finer, in_specs=in_specs, out_specs=out_specs, check_vma=False)
```

```python
import functools

import jax
import jax.numpy as jnp
from jax import lax
from jax.experimental import pallas as pl
from jax.experimental.pallas import tpu as pltpu
from jax.sharding import Mesh
from jax.sharding import PartitionSpec as P

DP = ("dp_0", "dp_1", "dp_2", "dp_3")
EPS_NORM = 1e-06
EPS_SCALE = 1e-06
CLIP_RATIO = 0.9
SOFT = (6.579714691285096, -12.986868668454669, 12.191614515303863, -6.570949514891455, 1.970640660123473)
ROW_STEP = 256
SUB = 64
VMEM_LIMIT = 58 * 1024 * 1024
MESH_ID = pl.DeviceIdType.MESH


def soft_round(values):
    whole = jnp.round(values)
    rest = values - whole
    square = rest * rest
    poly = SOFT[4] * square + SOFT[3]
    for coefficient in (SOFT[2], SOFT[1], SOFT[0]):
        poly = poly * square + coefficient
    return whole + (rest * square) * poly


def fake_quant(values, step_size):
    return soft_round(jnp.clip(values / step_size, -8.0, 7.0)) * step_size


RING = 4
COLORS = ((0, 1, 2), (1, 2, 0), (2, 0, 1))


class Gather:
    def __init__(self, buffer, place, send, recv, areas, parts):
        self.buffer, self.place, self.send, self.recv = buffer, place, send, recv
        self.half = buffer.shape[4] // 2
        self.areas, self.parts = areas, parts
        self.partner = {DP[3]: 1 - place[3]}
        self.pending = {None: []}
        self.state = {}
        self.counter = 0

    def view(self, color, position, phase, part, side=None):
        which, first_row, count, start, width = self.areas[color]
        order = COLORS[which]
        done = order[:phase]
        cols = pl.ds(pl.multiple_of(self.place[3] * self.half + start, 128), width)
        index = [self.place[k] for k in range(3)]
        for k in done:
            index[k] = slice(None)
        index[order[phase]] = position
        if side is not None:
            index[done[0]] = pl.ds(2 * side, 2)
        rows = pl.ds(first_row, count)
        if part is not None:
            count = count // self.parts
            rows = pl.ds(first_row + part * count, count)
        return self.buffer.at[index[0], index[1], index[2], rows, cols]

    def copy(self, view, peer, part):
        slot = self.counter
        self.counter += 1
        copy = pltpu.make_async_remote_copy(
            src_ref=view, dst_ref=view, send_sem=self.send.at[slot], recv_sem=self.recv.at[slot],
            device_id=peer, device_id_type=MESH_ID,
        )
        copy.start()
        self.pending.setdefault(part, []).append((copy, peer is self.partner))
        return copy

    def ring(self, color, phase):
        axis = COLORS[self.areas[color][0]][phase]
        own = self.place[axis]
        return axis, own, lax.rem(own + 1, RING), lax.rem(own + 2, RING), lax.rem(own + RING - 1, RING)

    def begin(self, phase, part=None):
        for color in range(len(self.areas)):
            axis, own, above, across, below = self.ring(color, phase)
            block = self.view(color, own, phase, part)
            copies = [self.copy(block, {DP[axis]: above}, part), self.copy(block, {DP[axis]: below}, part)]
            if phase == 0:
                copies.append(self.copy(block, {DP[axis]: across}, part))
            self.state[phase, color, part] = copies

    def relay(self, phase, part=None):
        for color in range(len(self.areas)):
            axis, own, above, across, below = self.ring(color, phase)
            from_below, from_above = self.state[phase, color, part]
            from_below.wait_recv()
            first = self.copy(self.view(color, below, phase, part, 0), {DP[axis]: above}, part)
            self.copy(self.view(color, below, phase, part), self.partner, part)
            from_above.wait_recv()
            second = self.copy(self.view(color, above, phase, part, 1), {DP[axis]: below}, part)
            self.copy(self.view(color, above, phase, part), self.partner, part)
            self.state[phase, color, part] = [first, second]

    def finish(self, phase, part=None):
        for color in range(len(self.areas)):
            axis, own, above, across, below = self.ring(color, phase)
            for copy in self.state[phase, color, part]:
                copy.wait_recv()
            self.copy(self.view(color, across, phase, part), self.partner, part)
            if phase == 0:
                self.copy(self.view(color, below, phase, part), self.partner, part)
                self.copy(self.view(color, above, phase, part), self.partner, part)

    def drain(self, part=None):
        for copy, kept in self.pending.pop(part, []):
            copy.wait_send()
            if kept:
                copy.wait_recv()


def bands(first_row, rows, first_column, widths):
    return [
        (k, first_row, rows, first_column + sum(widths[:k]), width) for k, width in enumerate(widths)
    ]


def gather_slots(areas, parts):
    return areas * (6 + 7 + 7 * parts)


NEAR = [(dy, dc) for dy in range(4) for dc in range(2) if (dy, dc) != (0, 0)]
FAR = [(dx, dz) for dx in range(4) for dz in range(4) if (dx, dz) != (0, 0)]


def near_peers(place):
    return [{DP[2]: lax.rem(place[2] + dy, 4), DP[3]: lax.rem(place[3] + dc, 2)} for dy, dc in NEAR]


def far_peers(place):
    return [{DP[0]: lax.rem(place[0] + dx, 4), DP[1]: lax.rem(place[1] + dz, 4)} for dx, dz in FAR]


class Exchange:
    def __init__(self, combine, place, buffers):
        self.combine, self.place = combine, place
        self.source, self.near, self.mid, self.far = buffers[:4]
        self.near_send, self.near_recv, self.far_send, self.far_recv = buffers[4:]

    def share(self, source, slots, me, peers, send, recv):
        slots[me] = source[...]
        copies = [
            pltpu.make_async_remote_copy(
                src_ref=source, dst_ref=slots.at[me], send_sem=send.at[k], recv_sem=recv.at[k],
                device_id=peer, device_id_type=MESH_ID,
            )
            for k, peer in enumerate(peers)
        ]
        for copy in copies:
            copy.start()
        return copies

    def total(self, slots, copies):
        for copy in copies:
            copy.wait()
        result = slots[0]
        for k in range(1, slots.shape[0]):
            result = self.combine(result, slots[k])
        return result

    def start(self, value):
        self.source[...] = value
        me = self.place[2] * 2 + self.place[3]
        self.copies = self.share(self.source, self.near, me, near_peers(self.place), self.near_send, self.near_recv)

    def turn(self):
        self.mid[...] = self.total(self.near, self.copies)
        me = self.place[0] * 4 + self.place[1]
        self.copies = self.share(self.mid, self.far, me, far_peers(self.place), self.far_send, self.far_recv)

    def finish(self):
        return self.total(self.far, self.copies)


def exchange_scratch(shape):
    return [
        pltpu.VMEM(shape, jnp.float32),
        pltpu.VMEM((8,) + shape, jnp.float32),
        pltpu.VMEM(shape, jnp.float32),
        pltpu.VMEM((16,) + shape, jnp.float32),
        pltpu.SemaphoreType.DMA((len(NEAR),)),
        pltpu.SemaphoreType.DMA((len(NEAR),)),
        pltpu.SemaphoreType.DMA((len(FAR),)),
        pltpu.SemaphoreType.DMA((len(FAR),)),
    ]


def quantize_rows(resid, act, square, error, first, count, sub=SUB):
    width = resid.shape[1]

    def step(index, carry):
        rows = pl.ds(pl.multiple_of(first + index * sub, sub), sub)
        squares = jnp.zeros((sub, 128), jnp.float32)
        tops = jnp.zeros((sub, 128), jnp.float32)
        for start in range(0, width, 128):
            part = resid[rows, start : start + 128]
            squares = squares + part * part
            tops = jnp.maximum(tops, jnp.abs(part))
        mean_sq = jnp.sum(squares, axis=1, keepdims=True) / width
        scale = lax.rsqrt(mean_sq + EPS_NORM)
        step_size = CLIP_RATIO * (jnp.max(tops, axis=1, keepdims=True) * scale) / 7.0 + EPS_SCALE
        gain = jnp.broadcast_to(scale / step_size, (sub, 128))
        wide_step = jnp.broadcast_to(step_size, (sub, 128))
        errors = jnp.zeros((sub, 128), jnp.float32)
        for start in range(0, width, 128):
            units = resid[rows, start : start + 128] * gain
            rounded = soft_round(jnp.minimum(jnp.maximum(units, -8.0), 7.0))
            gap = rounded - units
            errors = errors + gap * gap
            act[rows, start : start + 128] = (rounded * wide_step).astype(jnp.bfloat16)
        square[rows, :] = mean_sq
        error[rows, :] = jnp.sum(errors, axis=1, keepdims=True) * (step_size * step_size)
        return carry

    lax.fori_loop(0, count // sub, step, 0)


def quantize_mixed(mixed, gain, step_size, mix, error, first, count, sub=SUB):
    channels = mixed.shape[1]

    def step(index, carry):
        rows = pl.ds(pl.multiple_of(first + index * sub, sub), sub)
        errors = jnp.zeros((sub, 128), jnp.float32)
        for start in range(0, channels, 128):
            cols = slice(start, start + 128)
            units = mixed[rows, cols] * gain[:, cols]
            rounded = soft_round(jnp.minimum(jnp.maximum(units, -8.0), 7.0))
            gap = (rounded - units) * step_size[:, cols]
            errors = errors + gap * gap
            mix[rows, cols] = (rounded * step_size[:, cols]).astype(jnp.bfloat16)
        error[rows, :] = jnp.sum(errors, axis=1, keepdims=True)
        return carry

    lax.fori_loop(0, count // sub, step, 0)


def window_kernel(
    len_ref, all_len_ref, rotation_ref, value_ref, norm_ref, weight_ref, hidden_ref, out_ref, sum_ref,
    turn, full, product, left, mixed, mix, pair, wide, square, error, loss, top, gain, step_size,
    turn_send, turn_recv, ring_send, ring_recv, swap_send, swap_recv, local, *exchanges,
):
    place = [lax.axis_index(name) for name in DP]
    core = place[3]
    own_len = len_ref[((place[0] * RING + place[1]) * RING + place[2]) * 2 + core]
    tokens, width = hidden_ref.shape
    channels = mixed.shape[1]
    part = weight_ref.shape[1]
    shard = rotation_ref.shape[0]
    act = left
    barrier = pltpu.get_barrier_semaphore()
    peers = near_peers(place) + far_peers(place)
    for peer in peers:
        pl.semaphore_signal(barrier, inc=1, device_id=peer, device_id_type=MESH_ID)
    load = pltpu.make_async_copy(hidden_ref, left.at[pl.ds(0, tokens)], local.at[0])
    load.start()
    tops_max = Exchange(jnp.maximum, place, exchanges[0:8])
    ranges = [Exchange(jnp.maximum, place, exchanges[8:16]), Exchange(jnp.maximum, place, exchanges[16:24])]
    loss_sum = Exchange(jnp.add, place, exchanges[24:32])

    def swap(source, target, slot):
        copy = pltpu.make_async_remote_copy(
            src_ref=source, dst_ref=target, send_sem=swap_send.at[slot], recv_sem=swap_recv.at[slot],
            device_id={DP[3]: 1 - core}, device_id_type=MESH_ID,
        )
        copy.start()
        return copy

    both_shards = wide
    both_shards[core] = rotation_ref[...]
    small = [
        (norm_ref[k : k + 1, :] * value_ref[k].astype(jnp.float32)).astype(jnp.bfloat16).astype(jnp.float32)
        for k in range(2)
    ] + [weight_ref[k].astype(jnp.float32) for k in range(2)]
    left[tokens : tokens + 4 * part, :] = jnp.concatenate(small, axis=0).astype(jnp.bfloat16)
    pl.semaphore_wait(barrier, len(peers))
    swapped = swap(rotation_ref, both_shards.at[core], 0)
    swapped.wait()
    turn[place[0], place[1], place[2]] = jnp.concatenate(
        [both_shards[0].astype(jnp.float32), both_shards[1].astype(jnp.float32)], axis=0
    ).astype(jnp.bfloat16)
    early = Gather(turn, place, turn_send.at[0], turn_recv.at[0], bands(0, 2 * shard, 0, (256, 256, 256)), 1)
    third = (2 * shard // 3 + 7) // 8 * 8
    slices = [(0, 0, third), (1, third, third), (2, 2 * third, 2 * shard - 2 * third)]
    shared = [(which, row, rows, 1152, 128) for which, row, rows in slices]
    late = Gather(
        turn, place, turn_send.at[1], turn_recv.at[1], bands(0, 2 * shard, 768, (128, 128, 128)) + shared, 1
    )
    chunk = 256

    def columns(first_row, rows, first, count):
        def body(index, carry):
            for core_half in range(2):
                cols = pl.ds(pl.multiple_of(core_half * (width // 2) + first + index * chunk, chunk), chunk)
                block = turn[:, :, :, :, cols].reshape(width, chunk)
                product[first_row : first_row + rows, cols] = jnp.dot(
                    left[first_row : first_row + rows, :], block, preferred_element_type=jnp.float32
                )
            return carry

        lax.fori_loop(0, count, body, 0)

    early.begin(0)
    late.begin(0)
    early.finish(0)
    early.begin(1)
    late.finish(0)
    late.begin(1)
    early.relay(1)
    late.relay(1)
    early.finish(1)
    early.begin(2)
    load.wait()
    early.relay(2)
    late.finish(1)
    late.begin(2)
    early.finish(2)
    early.drain()
    late.relay(2)
    columns(0, tokens + 4 * part, 0, 2)
    late.finish(2)
    columns(0, tokens + 4 * part, 512, 1)
    late.drain()
    columns(tokens, 4 * part, 768, 2)

    def matrix(which):
        return product[tokens + which * part : tokens + (which + 1) * part, :]

    def combine(first):
        for k in (first, first + 1):
            both = jnp.concatenate([pair[0, k].astype(jnp.float32), pair[1, k].astype(jnp.float32)], axis=0)
            full[place[0], place[1], place[2], 2 * part * k : 2 * part * (k + 1), :] = both.astype(jnp.bfloat16)

    def weights(which):
        return full[:, :, :, 2 * part * which : 2 * part * (which + 1), :].reshape(channels, width)

    done = 0

    def rows_ahead(count):
        nonlocal done
        quantize_rows(product, act, square, error, done, count)
        done = done + count

    for k in range(2):
        value = matrix(k)
        value_top = jnp.max(jnp.abs(value), axis=1, keepdims=True)
        pair[core, k] = fake_quant(value, value_top / 7.0 + EPS_SCALE).astype(jnp.bfloat16)
    output_tops = jnp.concatenate(
        [jnp.max(jnp.abs(matrix(k)), axis=0, keepdims=True) for k in (2, 3)], axis=0
    )
    spot = pair.at[core, pl.ds(0, 2)]
    swapped = swap(spot, spot, 1)
    tops_max.start(output_tops)
    wide_first, wide_second = (512, 384, 384), (384, 512, 384)
    values = Gather(full, place, ring_send.at[0], ring_recv.at[0], bands(0, 4 * part, 0, wide_first), 2)
    outputs = Gather(full, place, ring_send.at[1], ring_recv.at[1], bands(4 * part, 4 * part, 0, wide_second), 2)
    swapped.wait()
    combine(0)
    values.begin(0)
    columns(0, tokens, 768, 1)
    values.finish(0)
    values.begin(1)
    tops_max.turn()
    columns(0, tokens, 1024, 1)
    values.relay(1)
    rows_ahead(64)
    tops = tops_max.finish()
    for k in (2, 3):
        size = tops[k - 2 : k - 1, :] / 7.0 + EPS_SCALE
        pair[core, k] = fake_quant(matrix(k), size).astype(jnp.bfloat16)
    spot = pair.at[core, pl.ds(2, 2)]
    swapped = swap(spot, spot, 2)
    values.finish(1)
    swapped.wait()
    combine(2)
    outputs.begin(0)
    values.begin(2, 0)
    rows_ahead(192)
    outputs.finish(0)
    outputs.begin(1)
    rows_ahead(192)
    values.relay(2, 0)
    rows_ahead(64)
    outputs.relay(1)
    values.begin(2, 1)
    rows_ahead(256)
    values.finish(2, 0)
    outputs.finish(1)
    outputs.begin(2, 0)
    values.drain()
    values.drain(0)

    def live_rows(first, count):
        return first + lax.broadcasted_iota(jnp.int32, (count, 1), 0) < own_len

    def mix_block(first, which):
        rows = pl.ds(pl.multiple_of(first, ROW_STEP), ROW_STEP)
        block = lax.dot_general(
            act[rows, :], weights(which), (((1,), (1,)), ((), ())), preferred_element_type=jnp.float32
        )
        mixed[rows, :] = block
        seen = jnp.where(live_rows(first, ROW_STEP), jnp.abs(block), 0.0)
        top[...] = jnp.maximum(top[...], jnp.max(seen.reshape(ROW_STEP // 8, 8, channels), axis=0))

    def set_steps(vrange):
        sizes = CLIP_RATIO * vrange / 7.0 + EPS_SCALE
        step_size[...] = sizes
        gain[...] = 1.0 / sizes

    top[...] = jnp.zeros_like(top)
    loss[...] = square[...] * error[...]
    blocks = tokens // ROW_STEP

    def first(index, carry):
        mix_block(index * ROW_STEP, 0)
        return carry

    lax.fori_loop(0, blocks, first, 0)
    ranges[0].start(jnp.max(top[...], axis=0, keepdims=True))
    values.relay(2, 1)
    ranges[0].turn()
    outputs.relay(2, 0)
    outputs.begin(2, 1)
    values.finish(2, 1)
    outputs.finish(2, 0)
    set_steps(ranges[0].finish())
    values.drain(1)
    outputs.drain()
    outputs.drain(0)
    top[...] = jnp.zeros_like(top)

    def middle(index, carry):
        first = index * ROW_STEP
        rows = pl.ds(pl.multiple_of(first, ROW_STEP), ROW_STEP)
        quantize_mixed(mixed, gain, step_size, mix, error, first, ROW_STEP, 128)
        loss[rows, :] = loss[rows, :] + square[rows, :] * error[rows, :]
        product[rows, :] = product[rows, :] + jnp.dot(mix[rows, :], weights(2), preferred_element_type=jnp.float32)
        quantize_rows(product, act, square, error, first, ROW_STEP, 128)
        loss[rows, :] = loss[rows, :] + square[rows, :] * error[rows, :]
        mix_block(first, 1)
        return carry

    lax.fori_loop(0, 1, middle, 0)
    outputs.relay(2, 1)
    lax.fori_loop(1, blocks, middle, 0)
    outputs.finish(2, 1)
    ranges[1].start(jnp.max(top[...], axis=0, keepdims=True))
    outputs.drain(1)
    ranges[1].turn()
    set_steps(ranges[1].finish())
    quantize_mixed(mixed, gain, step_size, mix, error, 0, tokens, 128)
    kept = jnp.where(live_rows(0, tokens), loss[...] + square[...] * error[...], 0.0)
    loss_sum.start(jnp.broadcast_to(jnp.sum(kept, axis=0, keepdims=True), sum_ref.shape))

    def last(index, carry):
        first = index * ROW_STEP
        rows = pl.ds(pl.multiple_of(first, ROW_STEP), ROW_STEP)
        updated = product[rows, :] + jnp.dot(mix[rows, :], weights(3), preferred_element_type=jnp.float32)
        out_ref[rows, :] = jnp.where(live_rows(first, ROW_STEP), updated, 0.0).astype(jnp.bfloat16)
        return carry

    lax.fori_loop(0, 1, last, 0)
    loss_sum.turn()
    lax.fori_loop(1, blocks, last, 0)
    count = jnp.sum(all_len_ref[...].astype(jnp.float32), axis=1, keepdims=True)
    sum_ref[...] = loss_sum.finish() / count


def per_device(hidden, rotation, norm_gain, value_weight, output_weight, lengths):
    tokens, width = hidden.shape
    layers, part = output_weight.shape[0], output_weight.shape[1]
    channels = part * lax.axis_size(DP)
    shard = rotation.shape[0]
    column = pltpu.VMEM((tokens, 1), jnp.float32)
    cube = (RING, RING, RING)
    dma = pltpu.SemaphoreType.DMA
    scratch = [
        pltpu.VMEM(cube + (2 * shard, width), jnp.bfloat16),
        pltpu.VMEM(cube + (4 * layers * part, width), jnp.bfloat16),
        pltpu.VMEM((tokens + 2 * layers * part, width), jnp.float32),
        pltpu.VMEM((tokens + 2 * layers * part, width), jnp.bfloat16),
        pltpu.VMEM((tokens, channels), jnp.float32),
        pltpu.VMEM((tokens, channels), jnp.bfloat16),
        pltpu.VMEM((2, 2 * layers, part, width), jnp.bfloat16),
        pltpu.VMEM((2, shard, width), jnp.bfloat16),
        column, column, column,
        pltpu.VMEM((8, channels), jnp.float32),
        pltpu.VMEM((1, channels), jnp.float32),
        pltpu.VMEM((1, channels), jnp.float32),
        dma((2, gather_slots(6, 1))), dma((2, gather_slots(6, 1))),
        dma((2, gather_slots(3, 2))), dma((2, gather_slots(3, 2))),
        dma((3,)), dma((3,)), dma((1,)),
    ]
    for shape in ((layers, width), (1, channels), (1, channels), (1, 128)):
        scratch = scratch + exchange_scratch(shape)
    vmem = pl.BlockSpec(memory_space=pltpu.VMEM)
    out, total = pl.pallas_call(
        window_kernel,
        out_shape=[
            pltpu.VMEM((tokens, width), jnp.bfloat16),
            pltpu.VMEM((1, 128), jnp.float32),
        ],
        in_specs=[pl.BlockSpec(memory_space=pltpu.SMEM)] + [vmem] * 5 + [pl.BlockSpec(memory_space=pl.ANY)],
        out_specs=[vmem, vmem],
        scratch_shapes=scratch,
        compiler_params=pltpu.CompilerParams(collective_id=4, has_side_effects=True, vmem_limit_bytes=VMEM_LIMIT),
    )(
        lengths, lengths.reshape(1, -1), rotation, jnp.transpose(value_weight, (0, 2, 1)), norm_gain,
        output_weight, hidden,
    )
    return out, total[0, 0]


def solution(mesh):
    finer = Mesh(mesh.devices.reshape(4, 4, 4, 2), DP)
    in_specs = (P(DP, None), P(DP, None), P(), P(None, None, DP), P(None, DP, None), P())
    out_specs = (P(DP, None), P())
    return jax.shard_map(per_device, mesh=finer, in_specs=in_specs, out_specs=out_specs, check_vma=False)
```
